128 devices in a mesh: freq: 64 (over x, y, z_hi, core), depth: 2 (over z_lo).
Axes of the slice: x: 4, y: 4, z: 4 (z_hi: 2, z_lo: 2; z = z_hi * 2 + z_lo), core: 2. Of those that a mesh axis runs over, the one named last changes fastest.
Arguments:
- pressure_field: bfloat16 [8192, 16384], P('depth', 'freq'), may hold values from -6 to 6
- block_main: bfloat16 [8192, 3, 2, 128], P('depth'), may hold values from -0.15625 to 0.15625
- block_coupled: bfloat16 [8192, 3, 2, 128], P('depth'), may hold values from -0.15625 to 0.15625
- coupling: float32 [16384], P('freq'), may hold values from -3 to 3
- frequencies: float32 [8192], replicated, may hold values from 1 to 1024
- receivers: int32 [512], replicated, may hold values from 0 to 8191
- floors: int32 [4], replicated, may hold values from 2048 to 8191
Outputs:
- series: float32 [512, 2048], P('depth', 'freq')
The draws below stay inside these ranges and needn't reach their ends.
Inputs may be any that keep to these rules, and one draw needn't show every extreme that they name: `receivers`: any depth cells, repeats possible.
All inputs are finite; a program needn't handle non-finite values.
Results may differ from the reference program's by a relative error of at most 0.0061.
Values may be sent and summed in bfloat16 or wider, within the bound.
A program may use at most 256 MiB of HBM per device.

```python
import math
import jax
import jax.numpy as jnp
from jax import lax

NZ = 8192
BS = 128
NT = 2048
R = 512
STEPS = 4
F_DEV = 128
F = 8192
N_FREQ = 64


def touch_ends(array, key, smallest, largest):
    index_at = [jax.random.randint(jax.random.fold_in(key, axis), (), 0, length) for axis, length in enumerate(array.shape)]
    main_axis = array.shape.index(max(array.shape))
    next_to = index_at[:main_axis] + [(index_at[main_axis] + 1) % array.shape[main_axis]] + index_at[main_axis + 1:]
    return array.at[tuple(index_at)].set(smallest).at[tuple(next_to)].set(largest)


def levels(own_key, shape, cuts, least, top_value):
    level = 1.0
    for position, blocks in cuts:
        draws = jax.random.uniform(jax.random.fold_in(jax.random.fold_in(own_key, 6), position), (blocks,), jnp.float32, least / len(cuts), top_value / len(cuts))
        level = level * jnp.repeat(jnp.exp(draws), shape[position] // blocks).reshape((-1,) + (1,) * (len(shape) - 1 - position))
    return level


def gaussian(stream_key, dims, scale, reach, split=(), held_as=jnp.bfloat16):
    entries = scale * jax.random.normal(stream_key, dims, jnp.float32)
    if split:
        entries = entries * levels(stream_key, dims, split, -0.22, 0.18)
    return jnp.clip(entries, -reach, reach).astype(held_as)


def setup_inputs(seed: int = 0) -> dict:
    streams_of = jax.random.split(jax.random.key(seed), 8)
    return {
        "pressure_field": gaussian(streams_of[0], (NZ, 2 * F), 1.0, 6.0, ((0, 2), (1, 64))),
        "block_main": gaussian(streams_of[1], (NZ, 3, 2, BS), (12 * BS) ** -0.5, 0.15625, ((0, 2),)),
        "block_coupled": gaussian(streams_of[2], (NZ, 3, 2, BS), (12 * BS) ** -0.5, 0.15625, ((0, 2),)),
        "coupling": gaussian(streams_of[3], (2 * F,), 0.5, 3.0, ((0, 64),), jnp.float32),
        "frequencies": jnp.clip(jax.random.uniform(streams_of[4], (F,), jnp.float32, 1.0, 1024.0), 1.0, 1024.0),
        "receivers": touch_ends(jax.random.randint(streams_of[5], (R,), 0, NZ), jax.random.fold_in(streams_of[5], 1), 0, NZ - 1).astype(jnp.int32),
        "floors": touch_ends(jax.random.randint(streams_of[6], (STEPS,), NZ // 4, NZ), jax.random.fold_in(streams_of[6], 1), NZ // 4, NZ - 1).astype(jnp.int32),
    }


def apply_blocks(blocks, padded):
    block_count = blocks.shape[0]
    width = padded.shape[1]
    stacked = padded.reshape(block_count + 2, BS, width)
    neighbours = jnp.stack([stacked[:-2], stacked[1:-1], stacked[2:]], axis=1)
    product = jnp.einsum('bikrj,bkjc->rbic', blocks, neighbours, precision=lax.Precision.HIGHEST)
    real_part = product[0].reshape(block_count * BS, width)
    imag_part = product[1].reshape(block_count * BS, width // 2, 2)
    rotated = jnp.stack([-imag_part[..., 1], imag_part[..., 0]], axis=-1).reshape(block_count * BS, width)
    return real_part + rotated

def couple_terms(values, weights):
    height = values.shape[0]
    paired = values.reshape(height, -1, 2)
    wpair = weights.reshape(-1, 2)
    real_part = wpair[:, 0] * paired[..., 0] - wpair[:, 1] * paired[..., 1]
    imag_part = wpair[:, 0] * paired[..., 1] + wpair[:, 1] * paired[..., 0]
    return jnp.stack([real_part, imag_part], axis=-1).reshape(height, -1)

def make_basis(freq_values, sample_times):
    phase = jnp.mod(freq_values[:, None] * sample_times[None, :], jnp.float32(NT)) / jnp.float32(NT)
    angle = 2.0 * math.pi * phase
    stacked = jnp.stack([jnp.cos(angle), -jnp.sin(angle)], axis=1)
    return stacked.reshape(2 * freq_values.shape[0], sample_times.shape[0]).astype(jnp.bfloat16)

def reference(pressure_field, block_main, block_coupled, coupling, frequencies, receivers, floors):
    block_count = NZ // BS
    main_blocks = block_main.astype(jnp.float32).reshape(block_count, BS, 3, 2, BS)
    side_blocks = block_coupled.astype(jnp.float32).reshape(block_count, BS, 3, 2, BS)
    grouped = pressure_field.reshape(NZ, N_FREQ, 2 * F_DEV).transpose(1, 0, 2)
    pairs = coupling.reshape(N_FREQ, 2 * F_DEV)
    freq_groups = frequencies.reshape(N_FREQ, F_DEV)
    depth_index = jnp.arange(NZ, dtype=jnp.int32)
    sample_times = jnp.arange(NT, dtype=jnp.float32)

    def one_group(running, group_items):
        columns, weights, freq_values = group_items
        for step in range(STEPS):
            padded = jnp.pad(columns.astype(jnp.float32), ((BS, BS), (0, 0)))
            combined = apply_blocks(main_blocks, padded) + couple_terms(apply_blocks(side_blocks, padded), weights)
            damping = jnp.where(depth_index >= floors[step], 0.5, 1.0).astype(jnp.float32)
            columns = (damping[:, None] * combined).astype(jnp.bfloat16)
        picked = jnp.take(columns, receivers, axis=0)
        basis_table = make_basis(freq_values, sample_times)
        return (running + jnp.dot(picked, basis_table, preferred_element_type=jnp.float32), None)
    running, _ = lax.scan(one_group, jnp.zeros((R, NT), jnp.float32), (grouped, pairs, freq_groups))
    return running * (1.0 / math.sqrt(F))
```

```python
import functools
import math

import jax
import jax.numpy as jnp
from jax import lax
from jax.experimental import pallas as pl
from jax.experimental.pallas import tpu as pltpu
from jax.sharding import PartitionSpec as P

NT = 2048
STEPS = 4
NX, NY, NZH = 4, 4, 2
GROUP = 4

COS_TERMS = (1.0, -19.739208221435547, 64.93939208984375, -85.45665740966797,
             60.242130279541016, -26.4046688079834, 7.800131320953369, -1.453112244606018)
SIN_TERMS = (6.2831854820251465, -41.34170150756836, 81.6052474975586, -76.70580291748047,
             42.05775451660156, -15.086565017700195, 3.7813189029693604, -0.6207787394523621)

MESH = pl.DeviceIdType.MESH
F32 = jnp.float32
BF16 = jnp.bfloat16


def poly(terms, z):
    total = jnp.full_like(z, terms[-1])
    for term in terms[-2::-1]:
        total = total * z + F32(term)
    return total


def turn(y):
    p = y - jnp.floor(y)
    r = jnp.where(p > 0.5, p - 1.0, p)
    z = r * r
    return poly(COS_TERMS, z), r * poly(SIN_TERMS, z)


def kernel(depth_n, factor,
           field_hbm, main_hbm, side_hbm, coupling_hbm, freqs_hbm, receivers_hbm, floors, out,
           fbuf, raw_main, raw_side, spread0, spread1, spread2, spread3,
           ops0, ops1, ops2, ops3, w0, w1, final, halo, order_buf,
           coupling, freqs, receivers, weights, spots,
           picked, own, pick_in, sib_own, sib_in, owned,
           coarse, fine, basis_a, basis_b, keep, send1, recv1, send2, recv2, send3, recv3,
           field_sem, load_sem, small_sem, halo_send, halo_recv,
           pick_send, pick_recv, s1_send, s1_recv, s2_send, s2_recv, s3_send, s3_recv):
    rows, width = fbuf.shape
    half = width // 2
    bs = raw_main.shape[1]
    kc = 6
    nb = rows // bs
    bw = 2 * bs
    groups = nb // GROUP
    ops = (ops0, ops1, ops2, ops3)
    spreads = (spread0, spread1, spread2, spread3)
    w_bufs = (w0, w1)
    me_d = lax.axis_index("depth")
    me_f = lax.axis_index("freq")
    first_row = me_d * rows
    core = lax.rem(me_f, 2)
    z = lax.rem(me_f // 2, NZH)
    y = lax.rem(me_f // (2 * NZH), NY)
    x = me_f // (2 * NZH * NY)
    sibling = me_f + 1 - 2 * core

    def chip_of(ox, oy, oz):
        return (lax.rem(x + ox, NX) * NY + lax.rem(y + oy, NY)) * NZH + lax.rem(z + oz, NZH)

    def device_of(ox, oy, oz):
        return {"freq": chip_of(ox, oy, oz) * 2 + core}

    fch = fbuf.shape[0] // groups

    def field_copy(g):
        at = pl.ds(pl.multiple_of(g * fch, fch), fch)
        return pltpu.make_async_copy(field_hbm.at[at], fbuf.at[at], field_sem.at[g])

    def ops_copy(which, b):
        src, dst = ((main_hbm, raw_main), (side_hbm, raw_side))[which]
        at = pl.ds(pl.multiple_of(b * kc * bs, kc * bs), kc * bs)
        return pltpu.make_async_copy(src.at[at], dst.at[at], load_sem.at[which, b])

    small = [pltpu.make_async_copy(src, dst, small_sem.at[i]) for i, (src, dst) in enumerate(
        ((coupling_hbm, coupling), (freqs_hbm, freqs), (receivers_hbm, receivers)))]
    field_copy(0).start()
    small[0].start()

    def start_field(g, carry):
        field_copy(g).start()
        return carry
    lax.fori_loop(1, groups, start_field, 0)

    def start_ops(b, carry):
        ops_copy(0, b).start()
        ops_copy(1, b).start()
        return carry
    lax.fori_loop(0, nb, start_ops, 0)
    small[1].start()
    small[2].start()

    barrier = pltpu.get_barrier_semaphore()
    greeted = 0
    for off in range(1, depth_n):
        pl.semaphore_signal(barrier, inc=1, device_id={"depth": lax.rem(me_d + off, depth_n)},
                            device_id_type=MESH)
        greeted += 1
    peers = [{"freq": sibling}, device_of(0, 0, 1)]
    peers += [device_of(o, 0, 0) for o in range(1, NX)] + [device_of(0, o, 0) for o in range(1, NY)]
    for peer in peers:
        pl.semaphore_signal(barrier, inc=1, device_id=peer, device_id_type=MESH)
        greeted += 1

    from_col = lax.broadcasted_iota(jnp.int32, (width, width), 0)
    to_col = lax.broadcasted_iota(jnp.int32, (width, width), 1)
    wanted = jnp.where(to_col < half, 2 * to_col, 2 * (to_col - half) + 1)
    order_buf[...] = jnp.where(from_col == wanted, 1.0, 0.0).astype(BF16)

    def put_w(w_buf, b, re, im):
        base = pl.multiple_of((b + 1) * bw, bw)
        top, low = pl.ds(base, bs), pl.ds(pl.multiple_of(base + bs, bs), bs)
        w_buf[top, :half] = re
        w_buf[top, half:] = im
        w_buf[low, :half] = -im
        w_buf[low, half:] = re

    zero_edge = jnp.zeros((bw, width), BF16)
    for w_buf in w_bufs:
        w_buf[:bw, :] = zero_edge
        w_buf[(nb + 1) * bw:, :] = zero_edge

    def enter(g):
        field_copy(g).wait()
        at = pl.ds(pl.multiple_of(g * fch, fch), fch)
        got = jnp.dot(fbuf[at, :], order_buf[...], preferred_element_type=F32).astype(BF16)
        for i in range(GROUP):
            one = got[i * bs:(i + 1) * bs, :]
            put_w(w0, g * GROUP + i, one[:, :half], one[:, half:])

    enter(0)
    small[0].wait()
    c16 = jnp.broadcast_to(coupling[...], (16, width))
    high = c16.astype(BF16)
    rest = c16 - high.astype(F32)
    mid = rest.astype(BF16)
    low = (rest - mid.astype(F32)).astype(BF16)
    three = jnp.dot(jnp.concatenate([high, mid, low], axis=0), order_buf[...],
                    preferred_element_type=F32)
    weights[...] = (three[:8] + three[16:24]) + three[32:40]

    def enter_loop(g, carry):
        enter(g)
        return carry
    lax.fori_loop(1, groups, enter_loop, 0)

    pl.semaphore_wait(barrier, greeted)

    def halo_copy(step, side):
        edge = (1 if side == 0 else nb) * bw
        to = lax.rem(me_d + (depth_n - 1 if side == 0 else 1), depth_n)
        return pltpu.make_async_remote_copy(
            src_ref=w_bufs[step % 2].at[pl.ds(edge, bs)],
            dst_ref=halo.at[step, side],
            send_sem=halo_send.at[step, side],
            recv_sem=halo_recv.at[step, side],
            device_id={"depth": to},
            device_id_type=MESH,
        )

    has_above = me_d > 0
    has_below = me_d < depth_n - 1

    def halo_start(step):
        @pl.when(has_above)
        def _():
            halo_copy(step, 0).start()

        @pl.when(has_below)
        def _():
            halo_copy(step, 1).start()

    def halo_finish(step):
        @pl.when(has_above)
        def _():
            halo_copy(step, 0).wait_send()
            halo_copy(step, 1).wait_recv()
            put_w(w_bufs[step % 2], -1, halo[step, 1, :, :half], halo[step, 1, :, half:])

        @pl.when(has_below)
        def _():
            halo_copy(step, 1).wait_send()
            halo_copy(step, 0).wait_recv()
            put_w(w_bufs[step % 2], nb, halo[step, 0, :, :half], halo[step, 0, :, half:])

    halo_start(0)

    row_iota = lax.broadcasted_iota(jnp.int32, (bs, half), 0)

    def multiply(step, g, i):
        b = g * GROUP + i
        near = pl.ds(pl.multiple_of(b * bw, bw), 3 * bw)
        acc = jnp.dot(ops[i][g], w_bufs[step % 2][near, :], preferred_element_type=F32)
        m, c = acc[:bs], acc[bs:]
        wr = weights[0:1, :half]
        wi = weights[0:1, half:]
        re = m[:, :half] + wr * c[:, :half] - wi * c[:, half:]
        im = m[:, half:] + wr * c[:, half:] + wi * c[:, :half]
        damp = jnp.where(row_iota >= floors[step] - (first_row + b * bs), F32(0.5), F32(1.0))
        re = (damp * re).astype(BF16)
        im = (damp * im).astype(BF16)
        if step == STEPS - 1:
            at = pl.ds(pl.multiple_of(b * bs, bs), bs)
            final[at, :half] = re
            final[at, half:] = im
        else:
            put_w(w_bufs[1 - step % 2], b, re, im)

    def prepare(g, i):
        b = g * GROUP + i
        at = pl.ds(pl.multiple_of(b * kc * bs, kc * bs), kc * bs)
        for which, raw in enumerate((raw_main, raw_side)):
            ops_copy(which, b).wait()
            spread = spreads[2 * (i % 2) + which]
            spread[...] = raw[at, :].astype(F32)
            for piece in range(kc):
                ops[i][g, which * bs:(which + 1) * bs, piece * bs:(piece + 1) * bs] = spread[
                    pl.ds(piece, bs, stride=kc), :].astype(BF16)

    prepare(0, 0)
    prepare(0, 1)
    for i in range(1, GROUP):
        if i + 1 < GROUP:
            prepare(0, i + 1)
        else:
            prepare(1, 0)
        multiply(0, 0, i)

    def first_step(g, carry):
        for i in range(GROUP):
            if i + 1 < GROUP:
                prepare(g, i + 1)
            else:
                prepare(g + 1, 0)
            multiply(0, g, i)
        return carry

    lax.fori_loop(1, groups - 1, first_step, 0)
    for i in range(GROUP - 1):
        prepare(groups - 1, i + 1)
        multiply(0, groups - 1, i)
    halo_finish(0)
    multiply(0, 0, 0)
    multiply(0, groups - 1, GROUP - 1)
    small[1].wait()
    small[2].wait()
    for j in range(receivers.shape[0]):
        spots[j * bs:(j + 1) * bs, :] = jnp.broadcast_to(receivers[j:j + 1, :], (bs, bs)).T

    for step in range(1, STEPS):
        halo_start(step)
        for i in range(1, GROUP):
            multiply(step, 0, i)

        def inner(g, carry, step=step):
            for i in range(GROUP):
                multiply(step, g, i)
            return carry

        lax.fori_loop(1, groups - 1, inner, 0, unroll=2)
        for i in range(GROUP - 1):
            multiply(step, groups - 1, i)
        halo_finish(step)
        multiply(step, 0, 0)
        multiply(step, groups - 1, GROUP - 1)

    here = own.shape[0]
    chunk = min(rows, 1024)

    def pick(owner):
        at = pl.ds(pl.multiple_of(owner * here, here), here)
        local = spots[at, :] - first_row
        total = jnp.zeros((here, width), F32)
        for base in range(0, rows, chunk):
            marks = [
                jnp.where(local == lax.broadcasted_iota(jnp.int32, local.shape, 1) + (base + sub),
                          1.0, 0.0).astype(BF16)
                for sub in range(0, chunk, local.shape[1])
            ]
            total = total + jnp.dot(jnp.concatenate(marks, axis=1), final[base:base + chunk, :],
                                    preferred_element_type=F32)
        return total.astype(BF16)

    def move(src, dst, sems, at, to):
        return pltpu.make_async_remote_copy(
            src_ref=src, dst_ref=dst, send_sem=sems[0].at[at], recv_sem=sems[1].at[at],
            device_id=to, device_id_type=MESH)

    pick_sems = (pick_send, pick_recv)
    across = move(picked, pick_in, pick_sems, 0, {"depth": 1 - me_d})
    beside = move(own, sib_own, pick_sems, 1, {"freq": sibling})
    onward = move(pick_in, sib_in, pick_sems, 2, {"freq": sibling})
    picked[...] = pick(1 - me_d)
    across.start()
    own[...] = pick(me_d)
    beside.start()

    chips = NX * NY * NZH
    times = NT // (2 * chips)
    count = lax.broadcasted_iota(jnp.int32, (chips, half), 0).astype(F32)
    late = lax.broadcasted_iota(jnp.int32, (times, half), 0)
    late = (late + core * times).astype(F32)
    for h, line in enumerate((me_f, sibling)):
        tone = freqs[pl.ds(line, 1), :]
        at = slice(h * half, (h + 1) * half)
        cos, sin = turn((tone * count) * F32(1.0 / chips))
        coarse[0, :, at] = cos
        coarse[1, :, at] = -sin
        cos, sin = turn((tone * late) * F32(1.0 / NT))
        fine[0, :, at] = cos
        fine[1, :, at] = sin
    th = times // 2

    def basis_of(q, carry):
        ox, oy = q // NY, lax.rem(q, NY)
        for oz in range(NZH):
            chip = chip_of(ox, oy, oz)
            ca = coarse[0, pl.ds(chip, 1), :]
            na = coarse[1, pl.ds(chip, 1), :]
            for part, (basis, place) in enumerate(
                    ((basis_a, ox * NY + oy), (basis_b, oy * NX + ox))):
                at = pl.ds(pl.multiple_of((place * NZH + oz) * th, th), th)
                cb = fine[0, part * th:(part + 1) * th, :]
                sb = fine[1, part * th:(part + 1) * th, :]
                cos = (ca * cb + na * sb).astype(BF16)
                nsin = (na * cb - ca * sb).astype(BF16)
                for h in range(2):
                    basis[at, 2 * h * half:(2 * h + 1) * half] = cos[:, h * half:(h + 1) * half]
                    basis[at, (2 * h + 1) * half:(2 * h + 2) * half] = nsin[:, h * half:(h + 1) * half]
        return carry

    lax.fori_loop(0, NX * NY, basis_of, 0, unroll=4)

    across.wait()
    onward.start()
    owned[:, :width] = (own[...].astype(F32) + pick_in[...].astype(F32)).astype(BF16)
    beside.wait()
    onward.wait()
    owned[:, width:] = (sib_own[...].astype(F32) + sib_in[...].astype(F32)).astype(BF16)

    slab = NY * NZH * th
    piece = NZH * th
    s1, s2, s3 = (s1_send, s1_recv), (s2_send, s2_recv), (s3_send, s3_recv)

    def over(part, off):
        return device_of(off, 0, 0) if part == 0 else device_of(0, off, 0)

    def series(basis, at):
        return lax.dot_general(basis[at, :], owned[...], (((1,), (1,)), ((), ())),
                               preferred_element_type=F32)

    def first_copy(part, off):
        return move(send1.at[part, off - 1], recv1.at[part, off - 1], s1, (part, off - 1),
                    over(part, off))

    def second_copy(part, off):
        return move(send2.at[part, off - 1], recv2.at[part, off - 1], s2, (part, off - 1),
                    over(1 - part, off))

    def third_copy(part):
        return move(send3.at[part], recv3.at[part], s3, part, device_of(0, 0, 1))

    for part, basis in enumerate((basis_a, basis_b)):
        got = series(basis, slice(slab, NX * slab)).astype(BF16)
        for off in range(1, NX):
            send1[part, off - 1] = got[(off - 1) * slab:off * slab]
        for off in (2, 1, 3):
            first_copy(part, off).start()
    for part, basis in enumerate((basis_a, basis_b)):
        keep[part] = series(basis, slice(0, slab))
    for part in range(2):
        for off in range(1, NX):
            first_copy(part, off).wait()
        for off in (2, 1, 3, 0):
            at = slice(off * piece, (off + 1) * piece)
            total = keep[part, at, :]
            for k in range(NX - 1):
                total = total + recv1[part, k, at, :].astype(F32)
            if off:
                send2[part, off - 1] = total.astype(BF16)
                second_copy(part, off).start()
            else:
                keep[part, at, :] = total
    for part in range(2):
        for off in range(1, NY):
            second_copy(part, off).wait()
        for oz in (1, 0):
            at = slice(oz * th, (oz + 1) * th)
            total = keep[part, at, :]
            for k in range(NY - 1):
                total = total + recv2[part, k, at, :].astype(F32)
            if oz:
                send3[part] = total.astype(BF16)
                third_copy(part).start()
            else:
                keep[part, at, :] = total
    for part in range(2):
        third_copy(part).wait()
        out[part * th:(part + 1) * th, :] = (
            keep[part, :th, :] + recv3[part].astype(F32)) * factor


def local(depth_n, freq_n, pressure_field, block_main, block_coupled, coupling, frequencies,
          receivers, floors):
    rows, width = pressure_field.shape
    bs = block_main.shape[3]
    half = width // 2
    nb = rows // bs
    here = receivers.shape[0] // depth_n
    times = NT // freq_n
    factor = 1.0 / math.sqrt(frequencies.shape[0])
    vmem = pl.BlockSpec(memory_space=pltpu.VMEM)
    hbm = pl.BlockSpec(memory_space=pl.ANY)
    chips = NX * NY * NZH
    th = times // 2
    slab = NY * NZH * th
    dma = pltpu.SemaphoreType.DMA
    result = pl.pallas_call(
        functools.partial(kernel, depth_n, factor),
        out_shape=jax.ShapeDtypeStruct((times, here), F32),
        in_specs=[hbm] * 6 + [pl.BlockSpec(memory_space=pltpu.SMEM)],
        out_specs=vmem,
        scratch_shapes=[
            pltpu.VMEM((rows, width), BF16),
            pltpu.VMEM((rows * 6, bs), BF16),
            pltpu.VMEM((rows * 6, bs), BF16),
            *[pltpu.VMEM((6 * bs, bs), F32) for _ in range(4)],
            *[pltpu.VMEM((nb // GROUP, 2 * bs, 6 * bs), BF16) for _ in range(GROUP)],
            *[pltpu.VMEM(((nb + 2) * 2 * bs, width), BF16) for _ in range(2)],
            pltpu.VMEM((rows, width), BF16),
            pltpu.VMEM((STEPS, 2, bs, width), BF16),
            pltpu.VMEM((width, width), BF16),
            pltpu.VMEM((1, width), F32),
            pltpu.VMEM((frequencies.shape[0] // half, half), F32),
            pltpu.VMEM((receivers.shape[0] // bs, bs), jnp.int32),
            pltpu.VMEM((8, width), F32),
            pltpu.VMEM((receivers.shape[0], bs), jnp.int32),
            pltpu.VMEM((here, width), BF16),
            pltpu.VMEM((here, width), BF16),
            pltpu.VMEM((here, width), BF16),
            pltpu.VMEM((here, width), BF16),
            pltpu.VMEM((here, width), BF16),
            pltpu.VMEM((here, 2 * width), BF16),
            pltpu.VMEM((2, chips, width), F32),
            pltpu.VMEM((2, times, width), F32),
            pltpu.VMEM((NX * slab, 2 * width), BF16),
            pltpu.VMEM((NX * slab, 2 * width), BF16),
            pltpu.VMEM((2, slab, here), F32),
            pltpu.VMEM((2, NX - 1, slab, here), BF16),
            pltpu.VMEM((2, NX - 1, slab, here), BF16),
            pltpu.VMEM((2, NY - 1, NZH * th, here), BF16),
            pltpu.VMEM((2, NY - 1, NZH * th, here), BF16),
            pltpu.VMEM((2, th, here), BF16),
            pltpu.VMEM((2, th, here), BF16),
            dma((nb // GROUP,)),
            dma((2, nb)),
            dma((3,)),
            dma((STEPS, 2)),
            dma((STEPS, 2)),
            dma((3,)),
            dma((3,)),
            dma((2, NX - 1)),
            dma((2, NX - 1)),
            dma((2, NY - 1)),
            dma((2, NY - 1)),
            dma((2,)),
            dma((2,)),
        ],
        compiler_params=pltpu.CompilerParams(
            collective_id=0, has_side_effects=True, vmem_limit_bytes=64 * 1024 * 1024 - 128 * 1024
        ),
    )(
        pressure_field,
        block_main.reshape(rows * 6, bs),
        block_coupled.reshape(rows * 6, bs),
        coupling.reshape(1, width),
        frequencies.reshape(-1, half),
        receivers.reshape(-1, bs),
        floors,
    )
    return result.T


def solution(mesh):
    in_specs = (
        P("depth", "freq"),
        P("depth", None, None, None),
        P("depth", None, None, None),
        P("freq"),
        P(),
        P(),
        P(),
    )
    body = functools.partial(local, mesh.shape["depth"], mesh.shape["freq"])
    return jax.shard_map(body, mesh=mesh, in_specs=in_specs, out_specs=P("depth", "freq"),
                         check_vma=False)
```

```python
import functools
import math

import jax
import jax.numpy as jnp
from jax import lax
from jax.experimental import pallas as pl
from jax.experimental.pallas import tpu as pltpu
from jax.sharding import PartitionSpec as P

NT = 2048
STEPS = 4
NX, NY, NZH = 4, 4, 2
GROUP = 4
LATE = 2

COS_TERMS = (1.0, -19.739208221435547, 64.93939208984375, -85.45665740966797,
             60.242130279541016, -26.4046688079834, 7.800131320953369, -1.453112244606018)
SIN_TERMS = (6.2831854820251465, -41.34170150756836, 81.6052474975586, -76.70580291748047,
             42.05775451660156, -15.086565017700195, 3.7813189029693604, -0.6207787394523621)

MESH = pl.DeviceIdType.MESH
F32 = jnp.float32
BF16 = jnp.bfloat16


def poly(terms, z):
    total = jnp.full_like(z, terms[-1])
    for term in terms[-2::-1]:
        total = total * z + F32(term)
    return total


def turn(y):
    p = y - jnp.floor(y)
    r = jnp.where(p > 0.5, p - 1.0, p)
    z = r * r
    return poly(COS_TERMS, z), r * poly(SIN_TERMS, z)


def kernel(depth_n, factor,
           field_hbm, main_hbm, side_hbm, coupling_hbm, freqs_hbm, receivers_hbm, floors, out,
           fbuf, raw_main, raw_side, spread0, spread1, spread2, spread3,
           ops0, ops1, ops2, ops3, re0, re1, im0, im1, ni0, ni1,
           final_re, final_im, halo, order_buf,
           coupling, freqs, receivers, weights, spots,
           picked, own, pick_in, sib_own, sib_in, owned,
           coarse, fine, basis_a, basis_b, keep, send1, recv1, send2, recv2, send3, recv3,
           field_sem, load_sem, small_sem, halo_send, halo_recv,
           pick_send, pick_recv, s1_send, s1_recv, s2_send, s2_recv, s3_send, s3_recv):
    rows, width = fbuf.shape
    half = width // 2
    bs = raw_main.shape[1]
    kc = 6
    nb = rows // bs
    groups = nb // GROUP
    ops = (ops0, ops1, ops2, ops3)
    spreads = (spread0, spread1, spread2, spread3)
    re_bufs, im_bufs, ni_bufs = (re0, re1), (im0, im1), (ni0, ni1)
    me_d = lax.axis_index("depth")
    me_f = lax.axis_index("freq")
    first_row = me_d * rows
    core = lax.rem(me_f, 2)
    z = lax.rem(me_f // 2, NZH)
    y = lax.rem(me_f // (2 * NZH), NY)
    x = me_f // (2 * NZH * NY)
    sibling = me_f + 1 - 2 * core

    def chip_of(ox, oy, oz):
        return (lax.rem(x + ox, NX) * NY + lax.rem(y + oy, NY)) * NZH + lax.rem(z + oz, NZH)

    def device_of(ox, oy, oz):
        return {"freq": chip_of(ox, oy, oz) * 2 + core}

    fch = fbuf.shape[0] // groups

    def field_copy(g):
        at = pl.ds(pl.multiple_of(g * fch, fch), fch)
        return pltpu.make_async_copy(field_hbm.at[at], fbuf.at[at], field_sem.at[g])

    def ops_copies(g):
        count = GROUP * kc * bs
        at = pl.ds(pl.multiple_of(g * count, count), count)
        return [pltpu.make_async_copy(src.at[at], dst.at[at], load_sem.at[which, g])
                for which, (src, dst) in enumerate(((main_hbm, raw_main), (side_hbm, raw_side)))]

    small = [pltpu.make_async_copy(src, dst, small_sem.at[i]) for i, (src, dst) in enumerate(
        ((coupling_hbm, coupling), (freqs_hbm, freqs), (receivers_hbm, receivers)))]
    field_copy(0).start()
    field_copy(groups - 1).start()
    small[0].start()
    for copy in ops_copies(0):
        copy.start()
    field_copy(1).start()

    def start_group(g, carry):
        field_copy(g + 1).start()
        for copy in ops_copies(g):
            copy.start()
        return carry
    lax.fori_loop(1, groups - 2, start_group, 0)
    for g in (groups - 2, groups - 1):
        for copy in ops_copies(g):
            copy.start()
    small[1].start()
    small[2].start()

    barrier = pltpu.get_barrier_semaphore()
    greeted = 0
    for off in range(1, depth_n):
        pl.semaphore_signal(barrier, inc=1, device_id={"depth": lax.rem(me_d + off, depth_n)},
                            device_id_type=MESH)
        greeted += 1
    peers = [{"freq": sibling}, device_of(0, 0, 1)]
    peers += [device_of(o, 0, 0) for o in range(1, NX)] + [device_of(0, o, 0) for o in range(1, NY)]
    for peer in peers:
        pl.semaphore_signal(barrier, inc=1, device_id=peer, device_id_type=MESH)
        greeted += 1

    from_col = lax.broadcasted_iota(jnp.int32, (width, width), 0)
    to_col = lax.broadcasted_iota(jnp.int32, (width, width), 1)
    wanted = jnp.where(to_col < half, 2 * to_col, 2 * (to_col - half) + 1)
    order_buf[...] = jnp.where(from_col == wanted, 1.0, 0.0).astype(BF16)

    def put_w(parity, b, re, im):
        at = pl.ds(pl.multiple_of((b + 1) * bs, bs), bs)
        re_bufs[parity][at, :] = re
        im_bufs[parity][at, :] = im
        ni_bufs[parity][at, :] = -im

    zero_edge = jnp.zeros((bs, half), BF16)
    for buf in (re0, re1, im0, im1, ni0, ni1):
        buf[:bs, :] = zero_edge
        buf[(nb + 1) * bs:, :] = zero_edge

    def enter(g):
        at = pl.ds(pl.multiple_of(g * fch, fch), fch)
        got = jnp.dot(fbuf[at, :], order_buf[...], preferred_element_type=F32).astype(BF16)
        for i in range(GROUP):
            one = got[i * bs:(i + 1) * bs, :]
            put_w(0, g * GROUP + i, one[:, :half], one[:, half:])

    field_copy(0).wait()
    field_copy(groups - 1).wait()
    small[0].wait()
    enter(0)
    enter(groups - 1)
    c16 = jnp.broadcast_to(coupling[...], (16, width))
    high = c16.astype(BF16)
    rest = c16 - high.astype(F32)
    mid = rest.astype(BF16)
    low = (rest - mid.astype(F32)).astype(BF16)
    three = jnp.dot(jnp.concatenate([high, mid, low], axis=0), order_buf[...],
                    preferred_element_type=F32)
    weights[...] = (three[:8] + three[16:24]) + three[32:40]

    below = 1 - me_d
    edge = pl.ds(pl.multiple_of((below * (nb - 1) + 1) * bs, bs), bs)

    def halo_copies(step):
        return [pltpu.make_async_remote_copy(
            src_ref=bufs[step % 2].at[edge],
            dst_ref=halo.at[step, which],
            send_sem=halo_send.at[step, which],
            recv_sem=halo_recv.at[step, which],
            device_id={"depth": 1 - me_d},
            device_id_type=MESH,
        ) for which, bufs in enumerate((re_bufs, im_bufs))]

    def halo_start(step):
        for copy in halo_copies(step):
            copy.start()

    def halo_finish(step):
        for copy in halo_copies(step):
            copy.wait()
        put_w(step % 2, below * (nb + 1) - 1, halo[step, 0], halo[step, 1])

    row_iota = lax.broadcasted_iota(jnp.int32, (bs, half), 0)

    def multiply(step, g, i):
        b = g * GROUP + i
        parity = step % 2
        acc = None
        for k in range(3):
            at = pl.ds(pl.multiple_of((b + k) * bs, bs), bs)
            re, im, ni = re_bufs[parity][at, :], im_bufs[parity][at, :], ni_bufs[parity][at, :]
            near = jnp.concatenate([jnp.concatenate([re, im], axis=1),
                                    jnp.concatenate([ni, re], axis=1)], axis=0)
            block = jnp.concatenate([ops[i][g, 2 * k], ops[i][g, 2 * k + 1]], axis=1)
            part = jnp.dot(block, near, preferred_element_type=F32)
            acc = part if acc is None else acc + part
        m, c = acc[:bs], acc[bs:]
        wr = weights[0:1, :half]
        wi = weights[0:1, half:]
        re = m[:, :half] + wr * c[:, :half] - wi * c[:, half:]
        im = m[:, half:] + wr * c[:, half:] + wi * c[:, :half]
        damp = jnp.where(row_iota >= floors[step] - (first_row + b * bs), F32(0.5), F32(1.0))
        re = (damp * re).astype(BF16)
        im = (damp * im).astype(BF16)
        if step == STEPS - 1:
            at = pl.ds(pl.multiple_of(b * bs, bs), bs)
            final_re[at, :] = re
            final_im[at, :] = im
        else:
            put_w(1 - parity, b, re, im)

    def prepare(g, i):
        b = g * GROUP + i
        at = pl.ds(pl.multiple_of(b * kc * bs, kc * bs), kc * bs)
        for which, raw in enumerate((raw_main, raw_side)):
            spread = spreads[2 * (i % 2) + which]
            spread[...] = raw[at, :].astype(F32)
            for piece in range(kc):
                ops[i][g, piece, which * bs:(which + 1) * bs, :] = spread[
                    pl.ds(piece, bs, stride=kc), :].astype(BF16)

    def first_step(g, skip=0, last_field=None):
        for copy in ops_copies(g + 1):
            copy.wait()
        if last_field is None:
            field_copy(g + 2).wait()
        for i in range(GROUP):
            prepare(g + 1, i)
            if i >= skip:
                multiply(0, g, i)
        if last_field is None:
            enter(g + 2)

    for copy in ops_copies(0):
        copy.wait()
    field_copy(1).wait()
    for i in range(GROUP):
        prepare(0, i)
    enter(1)
    pl.semaphore_wait(barrier, greeted)
    halo_start(0)
    first_step(0, skip=1)

    def first_loop(g, carry):
        first_step(g)
        return carry

    lax.fori_loop(1, groups - 3, first_loop, 0)
    first_step(groups - 3, last_field=False)
    first_step(groups - 2, last_field=False)
    halo_finish(0)
    multiply(0, 0, 0)
    multiply(0, groups - 1, GROUP - 1)
    for i in range(GROUP - 1):
        multiply(0, groups - 1, i)
    small[1].wait()
    small[2].wait()
    for j in range(receivers.shape[0]):
        there = jnp.broadcast_to(receivers[j:j + 1, :], (bs, bs)).T - first_row
        spots[j * bs:(j + 1) * bs, :] = there.astype(jnp.int16)

    for step in range(1, STEPS):
        halo_start(step)
        for b in range(1, nb - 1 - LATE):
            multiply(step, b // GROUP, b % GROUP)
        halo_finish(step)
        multiply(step, 0, 0)
        multiply(step, groups - 1, GROUP - 1)
        for b in range(nb - 1 - LATE, nb - 1):
            multiply(step, b // GROUP, b % GROUP)

    here = own.shape[0]
    chunk = min(rows, 1024)

    def pick(owner):
        at = pl.ds(pl.multiple_of(owner * here, here), here)
        local = spots[at, :]
        lane = lax.broadcasted_iota(jnp.int32, local.shape, 1).astype(jnp.int16)
        total = None
        for base in range(0, rows, chunk):
            marks = [
                jnp.where(local == lane + jnp.int16(base + sub), BF16(1.0), BF16(0.0))
                for sub in range(0, chunk, bs)
            ]
            field = jnp.concatenate(
                [final_re[base:base + chunk, :], final_im[base:base + chunk, :]], axis=1)
            part = jnp.dot(jnp.concatenate(marks, axis=1), field, preferred_element_type=F32)
            total = part if total is None else total + part
        return total.astype(BF16)

    def move(src, dst, sems, at, to):
        return pltpu.make_async_remote_copy(
            src_ref=src, dst_ref=dst, send_sem=sems[0].at[at], recv_sem=sems[1].at[at],
            device_id=to, device_id_type=MESH)

    pick_sems = (pick_send, pick_recv)
    across = move(picked, pick_in, pick_sems, 0, {"depth": 1 - me_d})
    beside = move(own, sib_own, pick_sems, 1, {"freq": sibling})
    onward = move(pick_in, sib_in, pick_sems, 2, {"freq": sibling})
    picked[...] = pick(1 - me_d)
    across.start()
    own[...] = pick(me_d)
    beside.start()

    chips = NX * NY * NZH
    times = NT // (2 * chips)
    count = lax.broadcasted_iota(jnp.int32, (chips, half), 0).astype(F32)
    late = lax.broadcasted_iota(jnp.int32, (times, half), 0)
    late = (late + core * times).astype(F32)
    for h, line in enumerate((me_f, sibling)):
        tone = freqs[pl.ds(line, 1), :]
        at = slice(h * half, (h + 1) * half)
        cos, sin = turn((tone * count) * F32(1.0 / chips))
        coarse[0, :, at] = cos
        coarse[1, :, at] = -sin
        cos, sin = turn((tone * late) * F32(1.0 / NT))
        fine[0, :, at] = cos
        fine[1, :, at] = sin
    th = times // 2

    def basis_of(q, carry):
        ox, oy = q // NY, lax.rem(q, NY)
        for oz in range(NZH):
            chip = chip_of(ox, oy, oz)
            ca = coarse[0, pl.ds(chip, 1), :]
            na = coarse[1, pl.ds(chip, 1), :]
            for part, (basis, place) in enumerate(
                    ((basis_a, ox * NY + oy), (basis_b, oy * NX + ox))):
                at = pl.ds(pl.multiple_of((place * NZH + oz) * th, th), th)
                cb = fine[0, part * th:(part + 1) * th, :]
                sb = fine[1, part * th:(part + 1) * th, :]
                cos = (ca * cb + na * sb).astype(BF16)
                nsin = (na * cb - ca * sb).astype(BF16)
                for h in range(2):
                    basis[at, 2 * h * half:(2 * h + 1) * half] = cos[:, h * half:(h + 1) * half]
                    basis[at, (2 * h + 1) * half:(2 * h + 2) * half] = nsin[:, h * half:(h + 1) * half]
        return carry

    lax.fori_loop(0, NX * NY, basis_of, 0, unroll=4)

    across.wait()
    onward.start()
    owned[:, :width] = (own[...].astype(F32) + pick_in[...].astype(F32)).astype(BF16)
    beside.wait()
    onward.wait()
    owned[:, width:] = (sib_own[...].astype(F32) + sib_in[...].astype(F32)).astype(BF16)

    slab = NY * NZH * th
    piece = NZH * th
    s1, s2, s3 = (s1_send, s1_recv), (s2_send, s2_recv), (s3_send, s3_recv)

    def over(part, off):
        return device_of(off, 0, 0) if part == 0 else device_of(0, off, 0)

    def series(basis, at):
        return lax.dot_general(basis[at, :], owned[...], (((1,), (1,)), ((), ())),
                               preferred_element_type=F32)

    def first_copy(part, off):
        return move(send1.at[part, off - 1], recv1.at[part, off - 1], s1, (part, off - 1),
                    over(part, off))

    def second_copy(part, off):
        return move(send2.at[part, off - 1], recv2.at[part, off - 1], s2, (part, off - 1),
                    over(1 - part, off))

    def third_copy(part):
        return move(send3.at[part], recv3.at[part], s3, part, device_of(0, 0, 1))

    for part, basis in enumerate((basis_a, basis_b)):
        got = series(basis, slice(slab, NX * slab)).astype(BF16)
        for off in range(1, NX):
            send1[part, off - 1] = got[(off - 1) * slab:off * slab]
        for off in (2, 1, 3):
            first_copy(part, off).start()
    for part, basis in enumerate((basis_a, basis_b)):
        keep[part] = series(basis, slice(0, slab))
    for part in range(2):
        for off in range(1, NX):
            first_copy(part, off).wait()
        for off in (2, 1, 3, 0):
            at = slice(off * piece, (off + 1) * piece)
            total = keep[part, at, :]
            for k in range(NX - 1):
                total = total + recv1[part, k, at, :].astype(F32)
            if off:
                send2[part, off - 1] = total.astype(BF16)
                second_copy(part, off).start()
            else:
                keep[part, at, :] = total
    for part in range(2):
        for off in range(1, NY):
            second_copy(part, off).wait()
        for oz in (1, 0):
            at = slice(oz * th, (oz + 1) * th)
            total = keep[part, at, :]
            for k in range(NY - 1):
                total = total + recv2[part, k, at, :].astype(F32)
            if oz:
                send3[part] = total.astype(BF16)
                third_copy(part).start()
            else:
                keep[part, at, :] = total
    for part in range(2):
        third_copy(part).wait()
        out[part * th:(part + 1) * th, :] = (
            keep[part, :th, :] + recv3[part].astype(F32)) * factor


def local(depth_n, freq_n, pressure_field, block_main, block_coupled, coupling, frequencies,
          receivers, floors):
    rows, width = pressure_field.shape
    bs = block_main.shape[3]
    half = width // 2
    nb = rows // bs
    here = receivers.shape[0] // depth_n
    times = NT // freq_n
    factor = 1.0 / math.sqrt(frequencies.shape[0])
    vmem = pl.BlockSpec(memory_space=pltpu.VMEM)
    hbm = pl.BlockSpec(memory_space=pl.ANY)
    chips = NX * NY * NZH
    th = times // 2
    slab = NY * NZH * th
    dma = pltpu.SemaphoreType.DMA
    result = pl.pallas_call(
        functools.partial(kernel, depth_n, factor),
        out_shape=jax.ShapeDtypeStruct((times, here), F32),
        in_specs=[hbm] * 6 + [pl.BlockSpec(memory_space=pltpu.SMEM)],
        out_specs=vmem,
        scratch_shapes=[
            pltpu.VMEM((rows, width), BF16),
            pltpu.VMEM((rows * 6, bs), BF16),
            pltpu.VMEM((rows * 6, bs), BF16),
            *[pltpu.VMEM((6 * bs, bs), F32) for _ in range(4)],
            *[pltpu.VMEM((nb // GROUP, 6, 2 * bs, bs), BF16) for _ in range(GROUP)],
            *[pltpu.VMEM(((nb + 2) * bs, half), BF16) for _ in range(6)],
            pltpu.VMEM((rows, half), BF16),
            pltpu.VMEM((rows, half), BF16),
            pltpu.VMEM((STEPS, 2, bs, half), BF16),
            pltpu.VMEM((width, width), BF16),
            pltpu.VMEM((1, width), F32),
            pltpu.VMEM((frequencies.shape[0] // half, half), F32),
            pltpu.VMEM((receivers.shape[0] // bs, bs), jnp.int32),
            pltpu.VMEM((8, width), F32),
            pltpu.VMEM((receivers.shape[0], bs), jnp.int16),
            pltpu.VMEM((here, width), BF16),
            pltpu.VMEM((here, width), BF16),
            pltpu.VMEM((here, width), BF16),
            pltpu.VMEM((here, width), BF16),
            pltpu.VMEM((here, width), BF16),
            pltpu.VMEM((here, 2 * width), BF16),
            pltpu.VMEM((2, chips, width), F32),
            pltpu.VMEM((2, times, width), F32),
            pltpu.VMEM((NX * slab, 2 * width), BF16),
            pltpu.VMEM((NX * slab, 2 * width), BF16),
            pltpu.VMEM((2, slab, here), F32),
            pltpu.VMEM((2, NX - 1, slab, here), BF16),
            pltpu.VMEM((2, NX - 1, slab, here), BF16),
            pltpu.VMEM((2, NY - 1, NZH * th, here), BF16),
            pltpu.VMEM((2, NY - 1, NZH * th, here), BF16),
            pltpu.VMEM((2, th, here), BF16),
            pltpu.VMEM((2, th, here), BF16),
            dma((nb // GROUP,)),
            dma((2, nb // GROUP)),
            dma((3,)),
            dma((STEPS, 2)),
            dma((STEPS, 2)),
            dma((3,)),
            dma((3,)),
            dma((2, NX - 1)),
            dma((2, NX - 1)),
            dma((2, NY - 1)),
            dma((2, NY - 1)),
            dma((2,)),
            dma((2,)),
        ],
        compiler_params=pltpu.CompilerParams(
            collective_id=0, has_side_effects=True, vmem_limit_bytes=64 * 1024 * 1024 - 128 * 1024
        ),
    )(
        pressure_field,
        block_main.reshape(rows * 6, bs),
        block_coupled.reshape(rows * 6, bs),
        coupling.reshape(1, width),
        frequencies.reshape(-1, half),
        receivers.reshape(-1, bs),
        floors,
    )
    return result.T


def solution(mesh):
    in_specs = (
        P("depth", "freq"),
        P("depth", None, None, None),
        P("depth", None, None, None),
        P("freq"),
        P(),
        P(),
        P(),
    )
    body = functools.partial(local, mesh.shape["depth"], mesh.shape["freq"])
    return jax.shard_map(body, mesh=mesh, in_specs=in_specs, out_specs=P("depth", "freq"),
                         check_vma=False)
```

```python
import functools
import math

import jax
import jax.numpy as jnp
from jax import lax
from jax.experimental import pallas as pl
from jax.experimental.pallas import tpu as pltpu
from jax.sharding import PartitionSpec as P

NT = 2048
STEPS = 4
NX, NY, NZH = 4, 4, 2
GROUP = 4
LATE = 2

COS_TERMS = (1.0, -19.739208221435547, 64.93939208984375, -85.45665740966797,
             60.242130279541016, -26.4046688079834, 7.800131320953369, -1.453112244606018)
SIN_TERMS = (6.2831854820251465, -41.34170150756836, 81.6052474975586, -76.70580291748047,
             42.05775451660156, -15.086565017700195, 3.7813189029693604, -0.6207787394523621)

MESH = pl.DeviceIdType.MESH
F32 = jnp.float32
BF16 = jnp.bfloat16


def poly(terms, z):
    total = jnp.full_like(z, terms[-1])
    for term in terms[-2::-1]:
        total = total * z + F32(term)
    return total


def turn(y):
    p = y - jnp.floor(y)
    r = jnp.where(p > 0.5, p - 1.0, p)
    z = r * r
    return poly(COS_TERMS, z), r * poly(SIN_TERMS, z)


def kernel(depth_n, factor,
           field_hbm, main_hbm, side_hbm, coupling_hbm, freqs_hbm, receivers_hbm, floors, out,
           fbuf, raw_main, raw_side,
           ops0, ops1, ops2, ops3, re0, re1, im0, im1, ni0, ni1,
           final_re, final_im, halo, order_buf,
           coupling, freqs, receivers, weights, spots,
           picked, own, pick_in, sib_own, sib_in, owned,
           coarse, fine, basis_a, basis_b, keep, send1, recv1, send2, recv2, send3, recv3,
           field_sem, load_sem, small_sem, halo_send, halo_recv,
           pick_send, pick_recv, s1_send, s1_recv, s2_send, s2_recv, s3_send, s3_recv):
    rows, width = fbuf.shape
    half = width // 2
    bs = raw_main.shape[2]
    kc = 6
    nb = rows // bs
    groups = nb // GROUP
    ops = (ops0, ops1, ops2, ops3)
    re_bufs, im_bufs, ni_bufs = (re0, re1), (im0, im1), (ni0, ni1)
    me_d = lax.axis_index("depth")
    me_f = lax.axis_index("freq")
    first_row = me_d * rows
    core = lax.rem(me_f, 2)
    z = lax.rem(me_f // 2, NZH)
    y = lax.rem(me_f // (2 * NZH), NY)
    x = me_f // (2 * NZH * NY)
    sibling = me_f + 1 - 2 * core

    def chip_of(ox, oy, oz):
        return (lax.rem(x + ox, NX) * NY + lax.rem(y + oy, NY)) * NZH + lax.rem(z + oz, NZH)

    def device_of(ox, oy, oz):
        return {"freq": chip_of(ox, oy, oz) * 2 + core}

    fch = fbuf.shape[0] // groups

    def field_copy(g):
        at = pl.ds(pl.multiple_of(g * fch, fch), fch)
        return pltpu.make_async_copy(field_hbm.at[at], fbuf.at[at], field_sem.at[g])

    def ops_copies(g):
        at = pl.ds(g * GROUP, GROUP)
        return [pltpu.make_async_copy(src.at[at], dst.at[at], load_sem.at[which, g])
                for which, (src, dst) in enumerate(((main_hbm, raw_main), (side_hbm, raw_side)))]

    small = [pltpu.make_async_copy(src, dst, small_sem.at[i]) for i, (src, dst) in enumerate(
        ((coupling_hbm, coupling), (freqs_hbm, freqs), (receivers_hbm, receivers)))]
    field_copy(0).start()
    field_copy(groups - 1).start()
    small[0].start()
    for copy in ops_copies(0):
        copy.start()
    field_copy(1).start()

    def start_group(g, carry):
        field_copy(g + 1).start()
        for copy in ops_copies(g):
            copy.start()
        return carry
    lax.fori_loop(1, groups - 2, start_group, 0)
    for g in (groups - 2, groups - 1):
        for copy in ops_copies(g):
            copy.start()
    small[1].start()
    small[2].start()

    barrier = pltpu.get_barrier_semaphore()
    greeted = 0
    for off in range(1, depth_n):
        pl.semaphore_signal(barrier, inc=1, device_id={"depth": lax.rem(me_d + off, depth_n)},
                            device_id_type=MESH)
        greeted += 1
    peers = [{"freq": sibling}, device_of(0, 0, 1)]
    peers += [device_of(o, 0, 0) for o in range(1, NX)] + [device_of(0, o, 0) for o in range(1, NY)]
    for peer in peers:
        pl.semaphore_signal(barrier, inc=1, device_id=peer, device_id_type=MESH)
        greeted += 1

    from_col = lax.broadcasted_iota(jnp.int32, (width, width), 0)
    to_col = lax.broadcasted_iota(jnp.int32, (width, width), 1)
    wanted = jnp.where(to_col < half, 2 * to_col, 2 * (to_col - half) + 1)
    order_buf[...] = jnp.where(from_col == wanted, 1.0, 0.0).astype(BF16)

    def put_w(parity, b, re, im):
        at = pl.ds(pl.multiple_of((b + 1) * bs, bs), bs)
        re_bufs[parity][at, :] = re
        im_bufs[parity][at, :] = im
        ni_bufs[parity][at, :] = -im

    zero_edge = jnp.zeros((bs, half), BF16)
    for buf in (re0, re1, im0, im1, ni0, ni1):
        buf[:bs, :] = zero_edge
        buf[(nb + 1) * bs:, :] = zero_edge

    def enter(g):
        at = pl.ds(pl.multiple_of(g * fch, fch), fch)
        got = jnp.dot(fbuf[at, :], order_buf[...], preferred_element_type=F32).astype(BF16)
        for i in range(GROUP):
            one = got[i * bs:(i + 1) * bs, :]
            put_w(0, g * GROUP + i, one[:, :half], one[:, half:])

    field_copy(0).wait()
    field_copy(groups - 1).wait()
    small[0].wait()
    enter(0)
    enter(groups - 1)
    c16 = jnp.broadcast_to(coupling[...], (16, width))
    high = c16.astype(BF16)
    rest = c16 - high.astype(F32)
    mid = rest.astype(BF16)
    low = (rest - mid.astype(F32)).astype(BF16)
    three = jnp.dot(jnp.concatenate([high, mid, low], axis=0), order_buf[...],
                    preferred_element_type=F32)
    weights[...] = (three[:8] + three[16:24]) + three[32:40]

    below = 1 - me_d
    edge = pl.ds(pl.multiple_of((below * (nb - 1) + 1) * bs, bs), bs)

    def halo_copies(step):
        return [pltpu.make_async_remote_copy(
            src_ref=bufs[step % 2].at[edge],
            dst_ref=halo.at[step, which],
            send_sem=halo_send.at[step, which],
            recv_sem=halo_recv.at[step, which],
            device_id={"depth": 1 - me_d},
            device_id_type=MESH,
        ) for which, bufs in enumerate((re_bufs, im_bufs))]

    def halo_start(step):
        for copy in halo_copies(step):
            copy.start()

    def halo_finish(step):
        for copy in halo_copies(step):
            copy.wait()
        put_w(step % 2, below * (nb + 1) - 1, halo[step, 0], halo[step, 1])

    row_iota = lax.broadcasted_iota(jnp.int32, (bs, half), 0)

    def multiply(step, g, i):
        b = g * GROUP + i
        parity = step % 2
        acc = None
        for k in range(3):
            at = pl.ds(pl.multiple_of((b + k) * bs, bs), bs)
            re, im, ni = re_bufs[parity][at, :], im_bufs[parity][at, :], ni_bufs[parity][at, :]
            near = jnp.concatenate([jnp.concatenate([re, im], axis=1),
                                    jnp.concatenate([ni, re], axis=1)], axis=0)
            block = jnp.concatenate([ops[i][g, 2 * k], ops[i][g, 2 * k + 1]], axis=1)
            part = jnp.dot(block, near, preferred_element_type=F32)
            acc = part if acc is None else acc + part
        m, c = acc[:bs], acc[bs:]
        wr = weights[0:1, :half]
        wi = weights[0:1, half:]
        re = m[:, :half] + wr * c[:, :half] - wi * c[:, half:]
        im = m[:, half:] + wr * c[:, half:] + wi * c[:, :half]
        damp = jnp.where(row_iota >= floors[step] - (first_row + b * bs), F32(0.5), F32(1.0))
        re = (damp * re).astype(BF16)
        im = (damp * im).astype(BF16)
        if step == STEPS - 1:
            at = pl.ds(pl.multiple_of(b * bs, bs), bs)
            final_re[at, :] = re
            final_im[at, :] = im
        else:
            put_w(1 - parity, b, re, im)

    def prepare(g, i):
        for which, raw in enumerate((raw_main, raw_side)):
            for piece in range(kc):
                ops[i][g, piece, which * bs:(which + 1) * bs, :] = raw.at[
                    g * GROUP + i][pl.ds(piece, bs, stride=kc), :]

    def first_step(g, skip=0, last_field=None):
        for copy in ops_copies(g + 1):
            copy.wait()
        if last_field is None:
            field_copy(g + 2).wait()
        for i in range(GROUP):
            prepare(g + 1, i)
            if i >= skip:
                multiply(0, g, i)
        if last_field is None:
            enter(g + 2)

    for copy in ops_copies(0):
        copy.wait()
    field_copy(1).wait()
    for i in range(GROUP):
        prepare(0, i)
    enter(1)
    pl.semaphore_wait(barrier, greeted)
    halo_start(0)
    first_step(0, skip=1)

    def first_loop(g, carry):
        first_step(g)
        return carry

    lax.fori_loop(1, groups - 3, first_loop, 0)
    first_step(groups - 3, last_field=False)
    first_step(groups - 2, last_field=False)
    halo_finish(0)
    multiply(0, 0, 0)
    multiply(0, groups - 1, GROUP - 1)
    for i in range(GROUP - 1):
        multiply(0, groups - 1, i)
    small[1].wait()
    small[2].wait()
    for j in range(receivers.shape[0]):
        there = jnp.broadcast_to(receivers[j:j + 1, :], (bs, bs)).T - first_row
        spots[j * bs:(j + 1) * bs, :] = there.astype(jnp.int16)

    for step in range(1, STEPS):
        halo_start(step)
        for b in range(1, nb - 1 - LATE):
            multiply(step, b // GROUP, b % GROUP)
        halo_finish(step)
        multiply(step, 0, 0)
        multiply(step, groups - 1, GROUP - 1)
        for b in range(nb - 1 - LATE, nb - 1):
            multiply(step, b // GROUP, b % GROUP)

    here = own.shape[0]
    chunk = min(rows, 1024)

    def pick(owner, first, count):
        at = pl.ds(pl.multiple_of(owner * here + first, bs), count)
        local = spots[at, :]
        lane = lax.broadcasted_iota(jnp.int32, local.shape, 1).astype(jnp.int16)
        total = None
        for base in range(0, rows, chunk):
            marks = [
                jnp.where(local == lane + jnp.int16(base + sub), BF16(1.0), BF16(0.0))
                for sub in range(0, chunk, bs)
            ]
            field = jnp.concatenate(
                [final_re[base:base + chunk, :], final_im[base:base + chunk, :]], axis=1)
            part = jnp.dot(jnp.concatenate(marks, axis=1), field, preferred_element_type=F32)
            total = part if total is None else total + part
        return total.astype(BF16)

    def move(src, dst, sems, at, to):
        return pltpu.make_async_remote_copy(
            src_ref=src, dst_ref=dst, send_sem=sems[0].at[at], recv_sem=sems[1].at[at],
            device_id=to, device_id_type=MESH)

    pick_sems = (pick_send, pick_recv)
    across, onward = [], []
    for h in range(2):
        at = pl.ds(h * bs, bs)
        across.append(move(picked.at[at], pick_in.at[at], pick_sems, h, {"depth": 1 - me_d}))
        onward.append(move(pick_in.at[at], sib_in.at[at], pick_sems, 2 + h, {"freq": sibling}))
    beside = move(own, sib_own, pick_sems, 4, {"freq": sibling})
    for h in range(2):
        picked[h * bs:(h + 1) * bs, :] = pick(1 - me_d, h * bs, bs)
        across[h].start()
    own[...] = pick(me_d, 0, here)
    beside.start()

    chips = NX * NY * NZH
    times = NT // (2 * chips)
    count = lax.broadcasted_iota(jnp.int32, (chips, half), 0).astype(F32)
    late = lax.broadcasted_iota(jnp.int32, (times, half), 0)
    late = (late + core * times).astype(F32)
    for h, line in enumerate((me_f, sibling)):
        tone = freqs[pl.ds(line, 1), :]
        at = slice(h * half, (h + 1) * half)
        cos, sin = turn((tone * count) * F32(1.0 / chips))
        coarse[0, :, at] = cos
        coarse[1, :, at] = -sin
        cos, sin = turn((tone * late) * F32(1.0 / NT))
        fine[0, :, at] = cos
        fine[1, :, at] = sin
    th = times // 2

    def basis_of(q, carry):
        ox, oy = q // NY, lax.rem(q, NY)
        for oz in range(NZH):
            chip = chip_of(ox, oy, oz)
            ca = coarse[0, pl.ds(chip, 1), :]
            na = coarse[1, pl.ds(chip, 1), :]
            for part, (basis, place) in enumerate(
                    ((basis_a, ox * NY + oy), (basis_b, oy * NX + ox))):
                at = pl.ds(pl.multiple_of((place * NZH + oz) * th, th), th)
                cb = fine[0, part * th:(part + 1) * th, :]
                sb = fine[1, part * th:(part + 1) * th, :]
                cos = (ca * cb + na * sb).astype(BF16)
                nsin = (na * cb - ca * sb).astype(BF16)
                for h in range(2):
                    basis[at, 2 * h * half:(2 * h + 1) * half] = cos[:, h * half:(h + 1) * half]
                    basis[at, (2 * h + 1) * half:(2 * h + 2) * half] = nsin[:, h * half:(h + 1) * half]
        return carry

    lax.fori_loop(0, NX * NY, basis_of, 0, unroll=4)

    for h in range(2):
        across[h].wait()
        onward[h].start()
    owned[:, :width] = (own[...].astype(F32) + pick_in[...].astype(F32)).astype(BF16)
    beside.wait()
    for h in range(2):
        onward[h].wait()
    owned[:, width:] = (sib_own[...].astype(F32) + sib_in[...].astype(F32)).astype(BF16)

    slab = NY * NZH * th
    piece = NZH * th
    s1, s2, s3 = (s1_send, s1_recv), (s2_send, s2_recv), (s3_send, s3_recv)

    def over(part, off):
        return device_of(off, 0, 0) if part == 0 else device_of(0, off, 0)

    def series(basis, at):
        return lax.dot_general(basis[at, :], owned[...], (((1,), (1,)), ((), ())),
                               preferred_element_type=F32)

    def first_copy(part, off, late):
        at = pl.ds(0, piece) if late else pl.ds(piece, slab - piece)
        return move(send1.at[part, off - 1, at], recv1.at[part, off - 1, at], s1,
                    (part, off - 1, late), over(part, off))

    def second_copy(part, off, late):
        at = pl.ds(0, th) if late else pl.ds(th, piece - th)
        return move(send2.at[part, off - 1, at], recv2.at[part, off - 1, at], s2,
                    (part, off - 1, late), over(1 - part, off))

    def third_copy(part):
        return move(send3.at[part], recv3.at[part], s3, part, device_of(0, 0, 1))

    for part, basis in enumerate((basis_a, basis_b)):
        got = series(basis, slice(slab, NX * slab)).astype(BF16)
        for off in range(1, NX):
            send1[part, off - 1] = got[(off - 1) * slab:off * slab]
    for late in range(2):
        for off in (2, 1, 3):
            for part in range(2):
                first_copy(part, off, late).start()
    for part, basis in enumerate((basis_a, basis_b)):
        keep[part] = series(basis, slice(0, slab))

    def total_of(recv, count, part, first, size):
        at = slice(first, first + size)
        total = keep[part, at, :]
        for k in range(count):
            total = total + recv[part, k, at, :].astype(F32)
        return total

    for part in range(2):
        for off in range(1, NX):
            first_copy(part, off, 0).wait()
        for off in range(1, NY):
            send2[part, off - 1] = total_of(recv1, NX - 1, part, off * piece, piece).astype(BF16)
        for late in range(2):
            for off in (2, 1, 3):
                second_copy(part, off, late).start()
    for part in range(2):
        for off in range(1, NX):
            first_copy(part, off, 1).wait()
        keep[part, :piece, :] = total_of(recv1, NX - 1, part, 0, piece)
    for part in range(2):
        for off in range(1, NY):
            second_copy(part, off, 0).wait()
        send3[part] = total_of(recv2, NY - 1, part, th, th).astype(BF16)
        third_copy(part).start()
    for part in range(2):
        for off in range(1, NY):
            second_copy(part, off, 1).wait()
        keep[part, :th, :] = total_of(recv2, NY - 1, part, 0, th)
    for part in range(2):
        third_copy(part).wait()
        out[part * th:(part + 1) * th, :] = (
            keep[part, :th, :] + recv3[part].astype(F32)) * factor


def local(depth_n, freq_n, pressure_field, block_main, block_coupled, coupling, frequencies,
          receivers, floors):
    rows, width = pressure_field.shape
    bs = block_main.shape[3]
    half = width // 2
    nb = rows // bs
    here = receivers.shape[0] // depth_n
    times = NT // freq_n
    factor = 1.0 / math.sqrt(frequencies.shape[0])
    vmem = pl.BlockSpec(memory_space=pltpu.VMEM)
    hbm = pl.BlockSpec(memory_space=pl.ANY)
    chips = NX * NY * NZH
    th = times // 2
    slab = NY * NZH * th
    dma = pltpu.SemaphoreType.DMA
    result = pl.pallas_call(
        functools.partial(kernel, depth_n, factor),
        out_shape=jax.ShapeDtypeStruct((times, here), F32),
        in_specs=[hbm] * 6 + [pl.BlockSpec(memory_space=pltpu.SMEM)],
        out_specs=vmem,
        scratch_shapes=[
            pltpu.VMEM((rows, width), BF16),
            pltpu.VMEM((nb, 6 * bs, bs), BF16),
            pltpu.VMEM((nb, 6 * bs, bs), BF16),
            *[pltpu.VMEM((nb // GROUP, 6, 2 * bs, bs), BF16) for _ in range(GROUP)],
            *[pltpu.VMEM(((nb + 2) * bs, half), BF16) for _ in range(6)],
            pltpu.VMEM((rows, half), BF16),
            pltpu.VMEM((rows, half), BF16),
            pltpu.VMEM((STEPS, 2, bs, half), BF16),
            pltpu.VMEM((width, width), BF16),
            pltpu.VMEM((1, width), F32),
            pltpu.VMEM((frequencies.shape[0] // half, half), F32),
            pltpu.VMEM((receivers.shape[0] // bs, bs), jnp.int32),
            pltpu.VMEM((8, width), F32),
            pltpu.VMEM((receivers.shape[0], bs), jnp.int16),
            pltpu.VMEM((here, width), BF16),
            pltpu.VMEM((here, width), BF16),
            pltpu.VMEM((here, width), BF16),
            pltpu.VMEM((here, width), BF16),
            pltpu.VMEM((here, width), BF16),
            pltpu.VMEM((here, 2 * width), BF16),
            pltpu.VMEM((2, chips, width), F32),
            pltpu.VMEM((2, times, width), F32),
            pltpu.VMEM((NX * slab, 2 * width), BF16),
            pltpu.VMEM((NX * slab, 2 * width), BF16),
            pltpu.VMEM((2, slab, here), F32),
            pltpu.VMEM((2, NX - 1, slab, here), BF16),
            pltpu.VMEM((2, NX - 1, slab, here), BF16),
            pltpu.VMEM((2, NY - 1, NZH * th, here), BF16),
            pltpu.VMEM((2, NY - 1, NZH * th, here), BF16),
            pltpu.VMEM((2, th, here), BF16),
            pltpu.VMEM((2, th, here), BF16),
            dma((nb // GROUP,)),
            dma((2, nb // GROUP)),
            dma((3,)),
            dma((STEPS, 2)),
            dma((STEPS, 2)),
            dma((5,)),
            dma((5,)),
            dma((2, NX - 1, 2)),
            dma((2, NX - 1, 2)),
            dma((2, NY - 1, 2)),
            dma((2, NY - 1, 2)),
            dma((2,)),
            dma((2,)),
        ],
        compiler_params=pltpu.CompilerParams(
            collective_id=0, has_side_effects=True, vmem_limit_bytes=64 * 1024 * 1024 - 128 * 1024
        ),
    )(
        pressure_field,
        block_main.reshape(nb, 6 * bs, bs),
        block_coupled.reshape(nb, 6 * bs, bs),
        coupling.reshape(1, width),
        frequencies.reshape(-1, half),
        receivers.reshape(-1, bs),
        floors,
    )
    return result.T


def solution(mesh):
    in_specs = (
        P("depth", "freq"),
        P("depth", None, None, None),
        P("depth", None, None, None),
        P("freq"),
        P(),
        P(),
        P(),
    )
    body = functools.partial(local, mesh.shape["depth"], mesh.shape["freq"])
    return jax.shard_map(body, mesh=mesh, in_specs=in_specs, out_specs=P("depth", "freq"),
                         check_vma=False)
```

```python
import functools
import math

import jax
import jax.numpy as jnp
from jax import lax
from jax.experimental import pallas as pl
from jax.experimental.pallas import tpu as pltpu
from jax.sharding import PartitionSpec as P

NT = 2048
STEPS = 4
NX, NY, NZH = 4, 4, 2
GROUP = 4
LATE = 2

COS_TERMS = (1.0, -19.739208221435547, 64.93939208984375, -85.45665740966797,
             60.242130279541016, -26.4046688079834, 7.800131320953369, -1.453112244606018)
SIN_TERMS = (6.2831854820251465, -41.34170150756836, 81.6052474975586, -76.70580291748047,
             42.05775451660156, -15.086565017700195, 3.7813189029693604, -0.6207787394523621)

MESH = pl.DeviceIdType.MESH
F32 = jnp.float32
BF16 = jnp.bfloat16


def poly(terms, z):
    total = jnp.full_like(z, terms[-1])
    for term in terms[-2::-1]:
        total = total * z + F32(term)
    return total


def turn(y):
    p = y - jnp.floor(y)
    r = jnp.where(p > 0.5, p - 1.0, p)
    z = r * r
    return poly(COS_TERMS, z), r * poly(SIN_TERMS, z)


def kernel(depth_n, factor,
           field_hbm, main_hbm, side_hbm, coupling_hbm, freqs_hbm, receivers_hbm, floors_hbm, out,
           fbuf, raw_main, raw_side,
           ops0, ops1, ops2, ops3, re0, re1, im0, im1, ni0, ni1,
           final_re, final_im, halo, order_buf,
           coupling, freqs, receivers, floors, weights, near_rows, spots, grab_re, grab_im,
           picked, own, pick_in, sib_own, sib_in, owned,
           coarse, fine, basis_a, basis_b, keep, send1, recv1, send2, recv2, send3, recv3,
           field_sem, load_sem, small_sem, halo_send, halo_recv,
           pick_send, pick_recv, s1_send, s1_recv, s2_send, s2_recv, s3_send, s3_recv):
    rows, width = fbuf.shape
    half = width // 2
    bs = raw_main.shape[2]
    kc = 6
    nb = rows // bs
    groups = nb // GROUP
    ops = (ops0, ops1, ops2, ops3)
    re_bufs, im_bufs, ni_bufs = (re0, re1), (im0, im1), (ni0, ni1)
    me_d = lax.axis_index("depth")
    me_f = lax.axis_index("freq")
    first_row = me_d * rows
    core = lax.rem(me_f, 2)
    z = lax.rem(me_f // 2, NZH)
    y = lax.rem(me_f // (2 * NZH), NY)
    x = me_f // (2 * NZH * NY)
    sibling = me_f + 1 - 2 * core

    def chip_of(ox, oy, oz):
        return (lax.rem(x + ox, NX) * NY + lax.rem(y + oy, NY)) * NZH + lax.rem(z + oz, NZH)

    def device_of(ox, oy, oz):
        return {"freq": chip_of(ox, oy, oz) * 2 + core}

    fch = fbuf.shape[0] // groups

    def field_copy(g):
        at = pl.ds(pl.multiple_of(g * fch, fch), fch)
        return pltpu.make_async_copy(field_hbm.at[at], fbuf.at[at], field_sem.at[g])

    def ops_copies(g):
        at = pl.ds(g * GROUP, GROUP)
        return [pltpu.make_async_copy(src.at[at], dst.at[at], load_sem.at[which, g])
                for which, (src, dst) in enumerate(((main_hbm, raw_main), (side_hbm, raw_side)))]

    small = [pltpu.make_async_copy(src, dst, small_sem.at[i]) for i, (src, dst) in enumerate(
        ((coupling_hbm, coupling), (floors_hbm, floors), (freqs_hbm, freqs),
         (receivers_hbm, receivers)))]
    field_copy(0).start()
    field_copy(groups - 1).start()
    small[0].start()
    small[1].start()
    for copy in ops_copies(0):
        copy.start(priority=1)
    field_copy(1).start()

    def start_group(g, carry):
        field_copy(g + 1).start()
        for copy in ops_copies(g):
            copy.start(priority=1)
        return carry
    lax.fori_loop(1, groups - 2, start_group, 0)
    for g in (groups - 2, groups - 1):
        for copy in ops_copies(g):
            copy.start(priority=1)
    small[2].start()
    small[3].start()

    barrier = pltpu.get_barrier_semaphore()
    greeted = 0
    for off in range(1, depth_n):
        pl.semaphore_signal(barrier, inc=1, device_id={"depth": lax.rem(me_d + off, depth_n)},
                            device_id_type=MESH)
        greeted += 1
    peers = [{"freq": sibling}, device_of(0, 0, 1)]
    peers += [device_of(o, 0, 0) for o in range(1, NX)] + [device_of(0, o, 0) for o in range(1, NY)]
    for peer in peers:
        pl.semaphore_signal(barrier, inc=1, device_id=peer, device_id_type=MESH)
        greeted += 1

    for buf in (final_re, final_im):
        buf[rows:, :] = jnp.zeros((buf.shape[0] - rows, half), F32)

    from_col = lax.broadcasted_iota(jnp.int32, (width, width), 0)
    to_col = lax.broadcasted_iota(jnp.int32, (width, width), 1)
    wanted = jnp.where(to_col < half, 2 * to_col, 2 * (to_col - half) + 1)
    order_buf[...] = jnp.where(from_col == wanted, 1.0, 0.0).astype(BF16)

    def put_w(parity, b, re, im):
        at = pl.ds(pl.multiple_of((b + 1) * bs, bs), bs)
        re_bufs[parity][at, :] = re
        im_bufs[parity][at, :] = im
        ni_bufs[parity][at, :] = -im

    zero_edge = jnp.zeros((bs, half), BF16)
    for buf in (re0, re1, im0, im1, ni0, ni1):
        buf[:bs, :] = zero_edge
        buf[(nb + 1) * bs:, :] = zero_edge

    def enter(g):
        at = pl.ds(pl.multiple_of(g * fch, fch), fch)
        got = jnp.dot(fbuf[at, :], order_buf[...], preferred_element_type=F32).astype(BF16)
        for i in range(GROUP):
            one = got[i * bs:(i + 1) * bs, :]
            put_w(0, g * GROUP + i, one[:, :half], one[:, half:])

    field_copy(0).wait()
    field_copy(groups - 1).wait()
    small[0].wait()
    small[1].wait()
    enter(0)
    enter(groups - 1)
    c16 = jnp.broadcast_to(coupling[...], (16, width))
    high = c16.astype(BF16)
    rest = c16 - high.astype(F32)
    mid = rest.astype(BF16)
    low = (rest - mid.astype(F32)).astype(BF16)
    three = jnp.dot(jnp.concatenate([high, mid, low], axis=0), order_buf[...],
                    preferred_element_type=F32)
    weights[...] = (three[:8] + three[16:24]) + three[32:40]

    below = 1 - me_d
    edge = pl.ds(pl.multiple_of((below * (nb - 1) + 1) * bs, bs), bs)

    def halo_copies(step):
        return [pltpu.make_async_remote_copy(
            src_ref=bufs[step % 2].at[edge],
            dst_ref=halo.at[step, which],
            send_sem=halo_send.at[step, which],
            recv_sem=halo_recv.at[step, which],
            device_id={"depth": 1 - me_d},
            device_id_type=MESH,
        ) for which, bufs in enumerate((re_bufs, im_bufs))]

    def halo_start(step):
        for copy in halo_copies(step):
            copy.start()

    def halo_finish(step):
        for copy in halo_copies(step):
            copy.wait()
        put_w(step % 2, below * (nb + 1) - 1, halo[step, 0], halo[step, 1])

    row_iota = lax.broadcasted_iota(jnp.int32, (bs, half), 0)

    def piece_of(step, g, i, p):
        if step > 0:
            return ops[i][g, p]
        pair = [raw.at[g * GROUP + i][pl.ds(p, bs, stride=kc), :] for raw in (raw_main, raw_side)]
        piece = jnp.concatenate(pair, axis=0)
        ops[i][g, p] = piece
        return piece

    def multiply(step, g, i):
        b = g * GROUP + i
        parity = step % 2
        acc = None
        for k in range(3):
            at = pl.ds(pl.multiple_of((b + k) * bs, bs), bs)
            re, im, ni = re_bufs[parity][at, :], im_bufs[parity][at, :], ni_bufs[parity][at, :]
            near = jnp.concatenate([jnp.concatenate([re, im], axis=1),
                                    jnp.concatenate([ni, re], axis=1)], axis=0)
            block = jnp.concatenate(
                [piece_of(step, g, i, 2 * k), piece_of(step, g, i, 2 * k + 1)], axis=1)
            part = jnp.dot(block, near, preferred_element_type=F32)
            acc = part if acc is None else acc + part
        m, c = acc[:bs], acc[bs:]
        wr = weights[0:1, :half]
        wi = weights[0:1, half:]
        re = m[:, :half] + wr * c[:, :half] - wi * c[:, half:]
        im = m[:, half:] + wr * c[:, half:] + wi * c[:, :half]
        damp = jnp.where(row_iota >= floors[step] - (first_row + b * bs), F32(0.5), F32(1.0))
        re = damp * re
        im = damp * im
        if step == STEPS - 1:
            at = pl.ds(pl.multiple_of(b * bs, bs), bs)
            final_re[at, :] = re
            final_im[at, :] = im
        else:
            put_w(1 - parity, b, re.astype(BF16), im.astype(BF16))

    def first_step(g, skip=0, last_field=None):
        for copy in ops_copies(g):
            copy.wait()
        if last_field is None:
            field_copy(g + 2).wait()
        for i in range(GROUP):
            if i >= skip:
                multiply(0, g, i)
        if last_field is None:
            enter(g + 2)

    field_copy(1).wait()
    enter(1)
    pl.semaphore_wait(barrier, greeted)
    halo_start(0)
    first_step(0, skip=1)

    def first_loop(g, carry):
        first_step(g)
        return carry

    lax.fori_loop(1, groups - 3, first_loop, 0)
    first_step(groups - 3, last_field=False)
    first_step(groups - 2, last_field=False)
    for copy in ops_copies(groups - 1):
        copy.wait()
    halo_finish(0)
    multiply(0, 0, 0)
    multiply(0, groups - 1, GROUP - 1)
    for i in range(GROUP - 1):
        multiply(0, groups - 1, i)
    small[2].wait()
    small[3].wait()
    spot = receivers[...] - first_row
    inside = jnp.logical_and(spot >= 0, spot < rows)
    near_rows[...] = jnp.where(inside, spot, rows)
    spot_copies = [
        pltpu.make_async_copy(near_rows.at[j], spots.at[pl.ds(j * bs, bs)], small_sem.at[4 + j])
        for j in range(near_rows.shape[0])]
    for copy in spot_copies:
        copy.start()

    for step in range(1, STEPS):
        halo_start(step)
        for b in range(1, nb - 1 - LATE):
            multiply(step, b // GROUP, b % GROUP)
        halo_finish(step)
        multiply(step, 0, 0)
        multiply(step, groups - 1, GROUP - 1)
        for b in range(nb - 1 - LATE, nb - 1):
            multiply(step, b // GROUP, b % GROUP)

    here = own.shape[0]

    def pick(owner, h):
        def take(q, carry):
            for j in range(16):
                row = q * 16 + j
                spot = spots[owner * here + h * bs + row]
                grab_re[pl.ds(h * bs + row, 1), :] = final_re[pl.ds(spot, 1), :]
                grab_im[pl.ds(h * bs + row, 1), :] = final_im[pl.ds(spot, 1), :]
            return carry

        lax.fori_loop(0, bs // 16, take, 0, unroll=2)
        at = slice(h * bs, (h + 1) * bs)
        return jnp.concatenate([grab_re[at, :], grab_im[at, :]], axis=1).astype(BF16)

    for copy in spot_copies:
        copy.wait()

    def move(src, dst, sems, at, to):
        return pltpu.make_async_remote_copy(
            src_ref=src, dst_ref=dst, send_sem=sems[0].at[at], recv_sem=sems[1].at[at],
            device_id=to, device_id_type=MESH)

    pick_sems = (pick_send, pick_recv)
    across, onward = [], []
    for h in range(2):
        at = pl.ds(h * bs, bs)
        across.append(move(picked.at[at], pick_in.at[at], pick_sems, h, {"depth": 1 - me_d}))
        onward.append(move(pick_in.at[at], sib_in.at[at], pick_sems, 2 + h, {"freq": sibling}))
    beside = move(own, sib_own, pick_sems, 4, {"freq": sibling})
    for h in range(2):
        picked[h * bs:(h + 1) * bs, :] = pick(1 - me_d, h)
        across[h].start()
    for h in range(2):
        own[h * bs:(h + 1) * bs, :] = pick(me_d, h)
    beside.start()

    chips = NX * NY * NZH
    times = NT // (2 * chips)
    count = lax.broadcasted_iota(jnp.int32, (chips, half), 0).astype(F32)
    late = lax.broadcasted_iota(jnp.int32, (times, half), 0)
    late = (late + core * times).astype(F32)
    for h, line in enumerate((me_f, sibling)):
        tone = freqs[pl.ds(line, 1), :]
        at = slice(h * half, (h + 1) * half)
        cos, sin = turn((tone * count) * F32(1.0 / chips))
        coarse[0, :, at] = cos
        coarse[1, :, at] = -sin
        cos, sin = turn((tone * late) * F32(1.0 / NT))
        fine[0, :, at] = cos
        fine[1, :, at] = sin
    th = times // 2

    def basis_of(q, carry):
        ox, oy = q // NY, lax.rem(q, NY)
        for oz in range(NZH):
            chip = chip_of(ox, oy, oz)
            ca = coarse[0, pl.ds(chip, 1), :]
            na = coarse[1, pl.ds(chip, 1), :]
            for part, (basis, place) in enumerate(
                    ((basis_a, ox * NY + oy), (basis_b, oy * NX + ox))):
                at = pl.ds(pl.multiple_of((place * NZH + oz) * th, th), th)
                cb = fine[0, part * th:(part + 1) * th, :]
                sb = fine[1, part * th:(part + 1) * th, :]
                cos = (ca * cb + na * sb).astype(BF16)
                nsin = (na * cb - ca * sb).astype(BF16)
                for h in range(2):
                    basis[at, 2 * h * half:(2 * h + 1) * half] = cos[:, h * half:(h + 1) * half]
                    basis[at, (2 * h + 1) * half:(2 * h + 2) * half] = nsin[:, h * half:(h + 1) * half]
        return carry

    lax.fori_loop(0, NX * NY, basis_of, 0, unroll=4)

    for h in range(2):
        across[h].wait()
        onward[h].start()
    owned[:, :width] = (own[...].astype(F32) + pick_in[...].astype(F32)).astype(BF16)
    beside.wait()
    for h in range(2):
        onward[h].wait()
    owned[:, width:] = (sib_own[...].astype(F32) + sib_in[...].astype(F32)).astype(BF16)

    slab = NY * NZH * th
    piece = NZH * th
    s1, s2, s3 = (s1_send, s1_recv), (s2_send, s2_recv), (s3_send, s3_recv)

    def over(part, off):
        return device_of(off, 0, 0) if part == 0 else device_of(0, off, 0)

    def series(basis, at):
        return lax.dot_general(basis[at, :], owned[...], (((1,), (1,)), ((), ())),
                               preferred_element_type=F32)

    def first_copy(part, off, late):
        at = pl.ds(0, piece) if late else pl.ds(piece, slab - piece)
        return move(send1.at[part, off - 1, at], recv1.at[part, off - 1, at], s1,
                    (part, off - 1, late), over(part, off))

    def second_copy(part, off, late):
        at = pl.ds(0, th) if late else pl.ds(th, piece - th)
        return move(send2.at[part, off - 1, at], recv2.at[part, off - 1, at], s2,
                    (part, off - 1, late), over(1 - part, off))

    def third_copy(part):
        return move(send3.at[part], recv3.at[part], s3, part, device_of(0, 0, 1))

    for part, basis in enumerate((basis_a, basis_b)):
        got = series(basis, slice(slab, NX * slab)).astype(BF16)
        for off in range(1, NX):
            send1[part, off - 1] = got[(off - 1) * slab:off * slab]
    for late in range(2):
        for off in (2, 1, 3):
            for part in range(2):
                first_copy(part, off, late).start()
    for part, basis in enumerate((basis_a, basis_b)):
        keep[part] = series(basis, slice(0, slab))

    def total_of(recv, count, part, first, size):
        at = slice(first, first + size)
        total = keep[part, at, :]
        for k in range(count):
            total = total + recv[part, k, at, :].astype(F32)
        return total

    for part in range(2):
        for off in range(1, NX):
            first_copy(part, off, 0).wait()
        for off in range(1, NY):
            send2[part, off - 1] = total_of(recv1, NX - 1, part, off * piece, piece).astype(BF16)
        for late in range(2):
            for off in (2, 1, 3):
                second_copy(part, off, late).start()
    for part in range(2):
        for off in range(1, NX):
            first_copy(part, off, 1).wait()
        keep[part, :piece, :] = total_of(recv1, NX - 1, part, 0, piece)
    for part in range(2):
        for off in range(1, NY):
            second_copy(part, off, 0).wait()
        send3[part] = total_of(recv2, NY - 1, part, th, th).astype(BF16)
        third_copy(part).start()
    for part in range(2):
        for off in range(1, NY):
            second_copy(part, off, 1).wait()
        keep[part, :th, :] = total_of(recv2, NY - 1, part, 0, th)
    for part in range(2):
        third_copy(part).wait()
        out[part * th:(part + 1) * th, :] = (
            keep[part, :th, :] + recv3[part].astype(F32)) * factor


def local(depth_n, freq_n, pressure_field, block_main, block_coupled, coupling, frequencies,
          receivers, floors):
    rows, width = pressure_field.shape
    bs = block_main.shape[3]
    half = width // 2
    nb = rows // bs
    here = receivers.shape[0] // depth_n
    times = NT // freq_n
    factor = 1.0 / math.sqrt(frequencies.shape[0])
    vmem = pl.BlockSpec(memory_space=pltpu.VMEM)
    hbm = pl.BlockSpec(memory_space=pl.ANY)
    chips = NX * NY * NZH
    th = times // 2
    slab = NY * NZH * th
    dma = pltpu.SemaphoreType.DMA
    result = pl.pallas_call(
        functools.partial(kernel, depth_n, factor),
        out_shape=jax.ShapeDtypeStruct((times, here), F32),
        in_specs=[hbm] * 7,
        out_specs=vmem,
        scratch_shapes=[
            pltpu.VMEM((rows, width), BF16),
            pltpu.VMEM((nb, 6 * bs, bs), BF16),
            pltpu.VMEM((nb, 6 * bs, bs), BF16),
            *[pltpu.VMEM((nb // GROUP, 6, 2 * bs, bs), BF16) for _ in range(GROUP)],
            *[pltpu.VMEM(((nb + 2) * bs, half), BF16) for _ in range(6)],
            pltpu.VMEM((rows + 8, half), F32),
            pltpu.VMEM((rows + 8, half), F32),
            pltpu.VMEM((STEPS, 2, bs, half), BF16),
            pltpu.VMEM((width, width), BF16),
            pltpu.VMEM((1, width), F32),
            pltpu.VMEM((frequencies.shape[0] // half, half), F32),
            pltpu.VMEM((receivers.shape[0] // bs, bs), jnp.int32),
            pltpu.SMEM((STEPS,), jnp.int32),
            pltpu.VMEM((8, width), F32),
            pltpu.VMEM((receivers.shape[0] // bs, bs), jnp.int32),
            pltpu.SMEM((receivers.shape[0],), jnp.int32),
            pltpu.VMEM((here, half), F32),
            pltpu.VMEM((here, half), F32),
            pltpu.VMEM((here, width), BF16),
            pltpu.VMEM((here, width), BF16),
            pltpu.VMEM((here, width), BF16),
            pltpu.VMEM((here, width), BF16),
            pltpu.VMEM((here, width), BF16),
            pltpu.VMEM((here, 2 * width), BF16),
            pltpu.VMEM((2, chips, width), F32),
            pltpu.VMEM((2, times, width), F32),
            pltpu.VMEM((NX * slab, 2 * width), BF16),
            pltpu.VMEM((NX * slab, 2 * width), BF16),
            pltpu.VMEM((2, slab, here), F32),
            pltpu.VMEM((2, NX - 1, slab, here), BF16),
            pltpu.VMEM((2, NX - 1, slab, here), BF16),
            pltpu.VMEM((2, NY - 1, NZH * th, here), BF16),
            pltpu.VMEM((2, NY - 1, NZH * th, here), BF16),
            pltpu.VMEM((2, th, here), BF16),
            pltpu.VMEM((2, th, here), BF16),
            dma((nb // GROUP,)),
            dma((2, nb // GROUP)),
            dma((4 + receivers.shape[0] // bs,)),
            dma((STEPS, 2)),
            dma((STEPS, 2)),
            dma((5,)),
            dma((5,)),
            dma((2, NX - 1, 2)),
            dma((2, NX - 1, 2)),
            dma((2, NY - 1, 2)),
            dma((2, NY - 1, 2)),
            dma((2,)),
            dma((2,)),
        ],
        compiler_params=pltpu.CompilerParams(
            collective_id=0, has_side_effects=True, vmem_limit_bytes=64 * 1024 * 1024 - 128 * 1024
        ),
    )(
        pressure_field,
        block_main.reshape(nb, 6 * bs, bs),
        block_coupled.reshape(nb, 6 * bs, bs),
        coupling.reshape(1, width),
        frequencies.reshape(-1, half),
        receivers.reshape(-1, bs),
        floors,
    )
    return result.T


def solution(mesh):
    in_specs = (
        P("depth", "freq"),
        P("depth", None, None, None),
        P("depth", None, None, None),
        P("freq"),
        P(),
        P(),
        P(),
    )
    body = functools.partial(local, mesh.shape["depth"], mesh.shape["freq"])
    return jax.shard_map(body, mesh=mesh, in_specs=in_specs, out_specs=P("depth", "freq"),
                         check_vma=False)
```

```python
import functools
import math

import jax
import jax.numpy as jnp
from jax import lax
from jax.experimental import pallas as pl
from jax.experimental.pallas import tpu as pltpu
from jax.sharding import PartitionSpec as P

NT = 2048
STEPS = 4
NX, NY, NZH = 4, 4, 2
GROUP = 4
LATE = 2

COS_TERMS = (1.0, -19.739208221435547, 64.93939208984375, -85.45665740966797,
             60.242130279541016, -26.4046688079834, 7.800131320953369, -1.453112244606018)
SIN_TERMS = (6.2831854820251465, -41.34170150756836, 81.6052474975586, -76.70580291748047,
             42.05775451660156, -15.086565017700195, 3.7813189029693604, -0.6207787394523621)

MESH = pl.DeviceIdType.MESH
F32 = jnp.float32
BF16 = jnp.bfloat16


def poly(terms, z):
    total = jnp.full_like(z, terms[-1])
    for term in terms[-2::-1]:
        total = total * z + F32(term)
    return total


def turn(y):
    p = y - jnp.floor(y)
    r = jnp.where(p > 0.5, p - 1.0, p)
    z = r * r
    return poly(COS_TERMS, z), r * poly(SIN_TERMS, z)


def kernel(depth_n, factor,
           field_hbm, main_hbm, side_hbm, coupling_hbm, freqs_hbm, receivers_hbm, floors_hbm, out,
           fbuf, raw_main, raw_side,
           ops0, ops1, ops2, ops3, re0, re1, im0, im1, ni0, ni1,
           final_re, final_im, halo, order_buf,
           coupling, freqs, receivers, floors, weights, near_rows, spots, grab_re, grab_im,
           picked, own, pick_in, sib_own, owned,
           coarse, fine, basis_a, basis_b, keep, send1, recv1, send2, recv2, send3, recv3,
           field_sem, load_sem, small_sem, halo_send, halo_recv,
           pick_send, pick_recv, s1_send, s1_recv, s2_send, s2_recv, s3_send, s3_recv):
    rows, width = fbuf.shape
    half = width // 2
    bs = raw_main.shape[2]
    kc = 6
    nb = rows // bs
    groups = nb // GROUP
    ops = (ops0, ops1, ops2, ops3)
    re_bufs, im_bufs, ni_bufs = (re0, re1), (im0, im1), (ni0, ni1)
    me_d = lax.axis_index("depth")
    me_f = lax.axis_index("freq")
    first_row = me_d * rows
    core = lax.rem(me_f, 2)
    z = lax.rem(me_f // 2, NZH)
    y = lax.rem(me_f // (2 * NZH), NY)
    x = me_f // (2 * NZH * NY)
    sibling = me_f + 1 - 2 * core

    def chip_of(ox, oy, oz):
        return (lax.rem(x + ox, NX) * NY + lax.rem(y + oy, NY)) * NZH + lax.rem(z + oz, NZH)

    def device_of(ox, oy, oz, oc=0):
        return {"freq": chip_of(ox, oy, oz) * 2 + lax.rem(core + oc, 2)}

    fch = fbuf.shape[0] // groups

    def field_copy(g):
        at = pl.ds(pl.multiple_of(g * fch, fch), fch)
        return pltpu.make_async_copy(field_hbm.at[at], fbuf.at[at], field_sem.at[g])

    def ops_copies(g):
        at = pl.ds(g * GROUP, GROUP)
        return [pltpu.make_async_copy(src.at[at], dst.at[at], load_sem.at[which, g])
                for which, (src, dst) in enumerate(((main_hbm, raw_main), (side_hbm, raw_side)))]

    small = [pltpu.make_async_copy(src, dst, small_sem.at[i]) for i, (src, dst) in enumerate(
        ((coupling_hbm, coupling), (floors_hbm, floors), (freqs_hbm, freqs),
         (receivers_hbm, receivers)))]
    field_copy(0).start()
    field_copy(groups - 1).start()
    small[0].start()
    small[1].start()
    for copy in ops_copies(0):
        copy.start(priority=1)
    field_copy(1).start()

    def start_group(g, carry):
        field_copy(g + 1).start()
        for copy in ops_copies(g):
            copy.start(priority=1)
        return carry
    lax.fori_loop(1, groups - 2, start_group, 0)
    for g in (groups - 2, groups - 1):
        for copy in ops_copies(g):
            copy.start(priority=1)
    small[2].start()
    small[3].start()

    barrier = pltpu.get_barrier_semaphore()
    greeted = 0
    peers = [{"depth": 1 - me_d, "freq": me_f}, {"depth": 1 - me_d, "freq": sibling}]
    peers += [{"freq": sibling}, device_of(0, 0, 1), device_of(0, 0, 1, 1)]
    peers += [device_of(o, 0, 0) for o in range(1, NX)] + [device_of(0, o, 0) for o in range(1, NY)]
    for peer in peers:
        pl.semaphore_signal(barrier, inc=1, device_id=peer, device_id_type=MESH)
        greeted += 1

    for buf in (final_re, final_im):
        buf[rows:, :] = jnp.zeros((buf.shape[0] - rows, half), F32)

    from_col = lax.broadcasted_iota(jnp.int32, (width, width), 0)
    to_col = lax.broadcasted_iota(jnp.int32, (width, width), 1)
    wanted = jnp.where(to_col < half, 2 * to_col, 2 * (to_col - half) + 1)
    order_buf[...] = jnp.where(from_col == wanted, 1.0, 0.0).astype(BF16)

    def put_w(parity, b, re, im):
        at = pl.ds(pl.multiple_of((b + 1) * bs, bs), bs)
        re_bufs[parity][at, :] = re
        im_bufs[parity][at, :] = im
        ni_bufs[parity][at, :] = -im

    zero_edge = jnp.zeros((bs, half), BF16)
    for buf in (re0, re1, im0, im1, ni0, ni1):
        buf[:bs, :] = zero_edge
        buf[(nb + 1) * bs:, :] = zero_edge

    def enter(g):
        at = pl.ds(pl.multiple_of(g * fch, fch), fch)
        got = jnp.dot(fbuf[at, :], order_buf[...], preferred_element_type=F32).astype(BF16)
        for i in range(GROUP):
            one = got[i * bs:(i + 1) * bs, :]
            put_w(0, g * GROUP + i, one[:, :half], one[:, half:])

    field_copy(0).wait()
    field_copy(groups - 1).wait()
    small[0].wait()
    small[1].wait()
    enter(0)
    enter(groups - 1)
    c16 = jnp.broadcast_to(coupling[...], (16, width))
    high = c16.astype(BF16)
    rest = c16 - high.astype(F32)
    mid = rest.astype(BF16)
    low = (rest - mid.astype(F32)).astype(BF16)
    three = jnp.dot(jnp.concatenate([high, mid, low], axis=0), order_buf[...],
                    preferred_element_type=F32)
    weights[...] = (three[:8] + three[16:24]) + three[32:40]

    below = 1 - me_d
    edge = pl.ds(pl.multiple_of((below * (nb - 1) + 1) * bs, bs), bs)

    def halo_copies(step):
        return [pltpu.make_async_remote_copy(
            src_ref=bufs[step % 2].at[edge],
            dst_ref=halo.at[step, which],
            send_sem=halo_send.at[step, which],
            recv_sem=halo_recv.at[step, which],
            device_id={"depth": 1 - me_d},
            device_id_type=MESH,
        ) for which, bufs in enumerate((re_bufs, im_bufs))]

    def halo_start(step):
        for copy in halo_copies(step):
            copy.start()

    def halo_wait(step):
        for copy in halo_copies(step):
            copy.wait()

    def halo_put(step):
        put_w(step % 2, below * (nb + 1) - 1, halo[step, 0], halo[step, 1])

    row_iota = lax.broadcasted_iota(jnp.int32, (bs, half), 0)

    def piece_of(step, g, i, p):
        if step > 0:
            return ops[i][g, p]
        pair = [raw.at[g * GROUP + i][pl.ds(p, bs, stride=kc), :] for raw in (raw_main, raw_side)]
        piece = jnp.concatenate(pair, axis=0)
        ops[i][g, p] = piece
        return piece

    def multiply(step, g, i):
        b = g * GROUP + i
        parity = step % 2
        acc = None
        for k in range(3):
            at = pl.ds(pl.multiple_of((b + k) * bs, bs), bs)
            re, im, ni = re_bufs[parity][at, :], im_bufs[parity][at, :], ni_bufs[parity][at, :]
            near = jnp.concatenate([jnp.concatenate([re, im], axis=1),
                                    jnp.concatenate([ni, re], axis=1)], axis=0)
            block = jnp.concatenate(
                [piece_of(step, g, i, 2 * k), piece_of(step, g, i, 2 * k + 1)], axis=1)
            part = jnp.dot(block, near, preferred_element_type=F32)
            acc = part if acc is None else acc + part
        m, c = acc[:bs], acc[bs:]
        wr = weights[0:1, :half]
        wi = weights[0:1, half:]
        re = m[:, :half] + wr * c[:, :half] - wi * c[:, half:]
        im = m[:, half:] + wr * c[:, half:] + wi * c[:, :half]
        damp = jnp.where(row_iota >= floors[step] - (first_row + b * bs), F32(0.5), F32(1.0))
        re = damp * re
        im = damp * im
        if step == STEPS - 1:
            at = pl.ds(pl.multiple_of(b * bs, bs), bs)
            final_re[at, :] = re
            final_im[at, :] = im
        else:
            put_w(1 - parity, b, re.astype(BF16), im.astype(BF16))

    def first_step(g, skip=0, last_field=None):
        for copy in ops_copies(g):
            copy.wait()
        if last_field is None:
            field_copy(g + 2).wait()
        for i in range(GROUP):
            if i >= skip:
                multiply(0, g, i)
        if last_field is None:
            enter(g + 2)

    field_copy(1).wait()
    enter(1)
    pl.semaphore_wait(barrier, greeted)
    halo_start(0)
    first_step(0, skip=1)

    def first_loop(g, carry):
        first_step(g)
        return carry

    lax.fori_loop(1, groups - 3, first_loop, 0)
    first_step(groups - 3, last_field=False)
    first_step(groups - 2, last_field=False)
    for copy in ops_copies(groups - 1):
        copy.wait()
    halo_wait(0)
    for i in range(GROUP - 1):
        multiply(0, groups - 1, i)
    halo_put(0)
    multiply(0, 0, 0)
    multiply(0, groups - 1, GROUP - 1)
    small[2].wait()
    small[3].wait()
    spot = receivers[...] - first_row
    inside = jnp.logical_and(spot >= 0, spot < rows)
    near_rows[...] = jnp.where(inside, spot, rows)
    spot_copies = [
        pltpu.make_async_copy(near_rows.at[j], spots.at[pl.ds(j * bs, bs)], small_sem.at[4 + j])
        for j in range(near_rows.shape[0])]
    for copy in spot_copies:
        copy.start()

    for step in range(1, STEPS):
        halo_start(step)
        for b in range(1, nb - 1 - LATE):
            multiply(step, b // GROUP, b % GROUP)
        halo_wait(step)
        for b in range(nb - 1 - LATE, nb - 1):
            multiply(step, b // GROUP, b % GROUP)
        halo_put(step)
        multiply(step, 0, 0)
        multiply(step, groups - 1, GROUP - 1)

    here = 2 * bs

    def pick(owner, side):
        base = owner * here + lax.rem(core + side, 2) * bs

        def take(q, carry):
            for j in range(16):
                row = q * 16 + j
                spot = spots[base + row]
                grab_re[pl.ds(row, 1), :] = final_re[pl.ds(spot, 1), :]
                grab_im[pl.ds(row, 1), :] = final_im[pl.ds(spot, 1), :]
            return carry

        lax.fori_loop(0, bs // 16, take, 0, unroll=2)
        return jnp.concatenate([grab_re[...], grab_im[...]], axis=1).astype(BF16)

    for copy in spot_copies:
        copy.wait()

    def move(src, dst, sems, at, to):
        return pltpu.make_async_remote_copy(
            src_ref=src, dst_ref=dst, send_sem=sems[0].at[at], recv_sem=sems[1].at[at],
            device_id=to, device_id_type=MESH)

    pick_sems = (pick_send, pick_recv)
    across = []
    for side, line in enumerate((me_f, sibling)):
        across.append(move(picked.at[side], pick_in.at[side], pick_sems, side,
                           {"depth": 1 - me_d, "freq": line}))
    beside = move(own.at[1], sib_own, pick_sems, 2, {"freq": sibling})
    for side in range(2):
        picked[side] = pick(1 - me_d, side)
        across[side].start()
    own[1] = pick(me_d, 1)
    beside.start()
    own[0] = pick(me_d, 0)

    chips = NX * NY * NZH
    times = NT // (2 * chips)
    count = lax.broadcasted_iota(jnp.int32, (chips, half), 0).astype(F32)
    late = lax.broadcasted_iota(jnp.int32, (2 * times, half), 0)
    late = jnp.where(late < times, late + core * times, late - core * times).astype(F32)
    for h, line in enumerate((me_f, sibling)):
        tone = freqs[pl.ds(line, 1), :]
        at = slice(h * half, (h + 1) * half)
        cos, sin = turn((tone * count) * F32(1.0 / chips))
        coarse[0, :, at] = cos
        coarse[1, :, at] = -sin
        cos, sin = turn((tone * late) * F32(1.0 / NT))
        fine[0, :, at] = cos
        fine[1, :, at] = sin
    th = times

    def basis_of(q, carry):
        ox, oy = q // NY, lax.rem(q, NY)
        for oz in range(NZH):
            chip = chip_of(ox, oy, oz)
            ca = coarse[0, pl.ds(chip, 1), :]
            na = coarse[1, pl.ds(chip, 1), :]
            for part, (basis, place) in enumerate(
                    ((basis_a, ox * NY + oy), (basis_b, oy * NX + ox))):
                at = pl.ds(pl.multiple_of((place * NZH + oz) * th, th), th)
                cb = fine[0, part * th:(part + 1) * th, :]
                sb = fine[1, part * th:(part + 1) * th, :]
                cos = (ca * cb + na * sb).astype(BF16)
                nsin = (na * cb - ca * sb).astype(BF16)
                for h in range(2):
                    basis[at, 2 * h * half:(2 * h + 1) * half] = cos[:, h * half:(h + 1) * half]
                    basis[at, (2 * h + 1) * half:(2 * h + 2) * half] = nsin[:, h * half:(h + 1) * half]
        return carry

    lax.fori_loop(0, NX * NY, basis_of, 0, unroll=2)

    for copy in across:
        copy.wait()
    beside.wait()
    for h, one in enumerate((own.at[0], sib_own)):
        owned[:, h * width:(h + 1) * width] = (
            one[...].astype(F32) + pick_in[h].astype(F32)).astype(BF16)

    slab = NY * NZH * th
    piece = NZH * th
    s1, s2, s3 = (s1_send, s1_recv), (s2_send, s2_recv), (s3_send, s3_recv)

    def over(part, off):
        return device_of(off, 0, 0) if part == 0 else device_of(0, off, 0)

    def series(basis, at):
        return lax.dot_general(basis[at, :], owned[...], (((1,), (1,)), ((), ())),
                               preferred_element_type=F32)

    def first_copy(part, off, late):
        at = pl.ds(0, piece) if late else pl.ds(piece, slab - piece)
        return move(send1.at[part, off - 1, at], recv1.at[part, off - 1, at], s1,
                    (part, off - 1, late), over(part, off))

    def second_copy(part, off, late):
        at = pl.ds(0, th) if late else pl.ds(th, piece - th)
        return move(send2.at[part, off - 1, at], recv2.at[part, off - 1, at], s2,
                    (part, off - 1, late), over(1 - part, off))

    third = [move(send3.at[k], recv3.at[k], s3, k, to) for k, to in enumerate(
        (device_of(0, 0, 1), device_of(0, 0, 1, 1), {"freq": sibling}))]

    for part, basis in enumerate((basis_a, basis_b)):
        got = series(basis, slice(slab, NX * slab)).astype(BF16)
        for off in range(1, NX):
            send1[part, off - 1] = got[(off - 1) * slab:off * slab]
    for late in range(2):
        for off in (2, 1, 3):
            for part in range(2):
                first_copy(part, off, late).start()
    for part, basis in enumerate((basis_a, basis_b)):
        keep[part] = series(basis, slice(0, slab))

    def total_of(recv, count, part, first, size):
        at = slice(first, first + size)
        total = keep[part, at, :]
        for k in range(count):
            total = total + recv[part, k, at, :].astype(F32)
        return total

    for part in range(2):
        for off in range(1, NX):
            first_copy(part, off, 0).wait()
        for off in range(1, NY):
            send2[part, off - 1] = total_of(recv1, NX - 1, part, off * piece, piece).astype(BF16)
        for late in range(2):
            for off in (2, 1, 3):
                second_copy(part, off, late).start()
    for part in range(2):
        for off in range(1, NX):
            first_copy(part, off, 1).wait()
        keep[part, :piece, :] = total_of(recv1, NX - 1, part, 0, piece)
    for part in range(2):
        for off in range(1, NY):
            second_copy(part, off, 0).wait()
        send3[part] = total_of(recv2, NY - 1, part, th, th).astype(BF16)
        third[part].start()
    for part in (1, 0):
        for off in range(1, NY):
            second_copy(part, off, 1).wait()
        total = total_of(recv2, NY - 1, part, 0, th)
        if part:
            send3[2] = total.astype(BF16)
            third[2].start()
        else:
            keep[0, :th, :] = total
    for copy in third:
        copy.wait()
    mine = (keep[0, :th, :] + recv3[0].astype(F32)) * factor
    theirs = (recv3[1].astype(F32) + recv3[2].astype(F32)) * factor
    first = core == 0
    out[:, :bs] = jnp.where(first, mine, theirs)
    out[:, bs:] = jnp.where(first, theirs, mine)


def local(depth_n, freq_n, pressure_field, block_main, block_coupled, coupling, frequencies,
          receivers, floors):
    rows, width = pressure_field.shape
    bs = block_main.shape[3]
    half = width // 2
    nb = rows // bs
    here = receivers.shape[0] // depth_n
    times = NT // freq_n
    factor = 1.0 / math.sqrt(frequencies.shape[0])
    vmem = pl.BlockSpec(memory_space=pltpu.VMEM)
    hbm = pl.BlockSpec(memory_space=pl.ANY)
    chips = NX * NY * NZH
    th = times
    slab = NY * NZH * th
    dma = pltpu.SemaphoreType.DMA
    result = pl.pallas_call(
        functools.partial(kernel, depth_n, factor),
        out_shape=jax.ShapeDtypeStruct((times, here), F32),
        in_specs=[hbm] * 7,
        out_specs=vmem,
        scratch_shapes=[
            pltpu.VMEM((rows, width), BF16),
            pltpu.VMEM((nb, 6 * bs, bs), BF16),
            pltpu.VMEM((nb, 6 * bs, bs), BF16),
            *[pltpu.VMEM((nb // GROUP, 6, 2 * bs, bs), BF16) for _ in range(GROUP)],
            *[pltpu.VMEM(((nb + 2) * bs, half), BF16) for _ in range(6)],
            pltpu.VMEM((rows + 8, half), F32),
            pltpu.VMEM((rows + 8, half), F32),
            pltpu.VMEM((STEPS, 2, bs, half), BF16),
            pltpu.VMEM((width, width), BF16),
            pltpu.VMEM((1, width), F32),
            pltpu.VMEM((frequencies.shape[0] // half, half), F32),
            pltpu.VMEM((receivers.shape[0] // bs, bs), jnp.int32),
            pltpu.SMEM((STEPS,), jnp.int32),
            pltpu.VMEM((8, width), F32),
            pltpu.VMEM((receivers.shape[0] // bs, bs), jnp.int32),
            pltpu.SMEM((receivers.shape[0],), jnp.int32),
            pltpu.VMEM((bs, half), F32),
            pltpu.VMEM((bs, half), F32),
            pltpu.VMEM((2, bs, width), BF16),
            pltpu.VMEM((2, bs, width), BF16),
            pltpu.VMEM((2, bs, width), BF16),
            pltpu.VMEM((bs, width), BF16),
            pltpu.VMEM((bs, 2 * width), BF16),
            pltpu.VMEM((2, chips, width), F32),
            pltpu.VMEM((2, 2 * times, width), F32),
            pltpu.VMEM((NX * slab, 2 * width), BF16),
            pltpu.VMEM((NX * slab, 2 * width), BF16),
            pltpu.VMEM((2, slab, bs), F32),
            pltpu.VMEM((2, NX - 1, slab, bs), BF16),
            pltpu.VMEM((2, NX - 1, slab, bs), BF16),
            pltpu.VMEM((2, NY - 1, NZH * th, bs), BF16),
            pltpu.VMEM((2, NY - 1, NZH * th, bs), BF16),
            pltpu.VMEM((3, th, bs), BF16),
            pltpu.VMEM((3, th, bs), BF16),
            dma((nb // GROUP,)),
            dma((2, nb // GROUP)),
            dma((4 + receivers.shape[0] // bs,)),
            dma((STEPS, 2)),
            dma((STEPS, 2)),
            dma((3,)),
            dma((3,)),
            dma((2, NX - 1, 2)),
            dma((2, NX - 1, 2)),
            dma((2, NY - 1, 2)),
            dma((2, NY - 1, 2)),
            dma((3,)),
            dma((3,)),
        ],
        compiler_params=pltpu.CompilerParams(
            collective_id=0, has_side_effects=True, vmem_limit_bytes=64 * 1024 * 1024 - 128 * 1024
        ),
    )(
        pressure_field,
        block_main.reshape(nb, 6 * bs, bs),
        block_coupled.reshape(nb, 6 * bs, bs),
        coupling.reshape(1, width),
        frequencies.reshape(-1, half),
        receivers.reshape(-1, bs),
        floors,
    )
    return result.T


def solution(mesh):
    in_specs = (
        P("depth", "freq"),
        P("depth", None, None, None),
        P("depth", None, None, None),
        P("freq"),
        P(),
        P(),
        P(),
    )
    body = functools.partial(local, mesh.shape["depth"], mesh.shape["freq"])
    return jax.shard_map(body, mesh=mesh, in_specs=in_specs, out_specs=P("depth", "freq"),
                         check_vma=False)
```

```python
import functools
import math

import jax
import jax.numpy as jnp
from jax import lax
from jax.experimental import pallas as pl
from jax.experimental.pallas import tpu as pltpu
from jax.sharding import PartitionSpec as P

NT = 2048
STEPS = 4
NX, NY, NZH = 4, 4, 2
GROUP = 4
LATE = 2

COS_TERMS = (1.0, -19.739208221435547, 64.93939208984375, -85.45665740966797,
             60.242130279541016, -26.4046688079834, 7.800131320953369, -1.453112244606018)
SIN_TERMS = (6.2831854820251465, -41.34170150756836, 81.6052474975586, -76.70580291748047,
             42.05775451660156, -15.086565017700195, 3.7813189029693604, -0.6207787394523621)

MESH = pl.DeviceIdType.MESH
F32 = jnp.float32
BF16 = jnp.bfloat16


def poly(terms, z):
    total = jnp.full_like(z, terms[-1])
    for term in terms[-2::-1]:
        total = total * z + F32(term)
    return total


def turn(y):
    p = y - jnp.floor(y)
    r = jnp.where(p > 0.5, p - 1.0, p)
    z = r * r
    return poly(COS_TERMS, z), r * poly(SIN_TERMS, z)


def kernel(depth_n, factor,
           field_hbm, main_hbm, side_hbm, coupling_hbm, freqs_hbm, receivers_hbm, floors_hbm, out,
           fbuf, raw_main, raw_side,
           ops0, ops1, ops2, ops3, re0, re1, im0, im1, ni0, ni1,
           final_re, final_im, halo, order_buf,
           coupling, freqs, receivers, floors, weights, near_rows, spots, grab_re, grab_im,
           picked, own, pick_in, sib_own, owned,
           coarse, fine, basis_a, basis_b, keep, send1, recv1, send2, recv2, send3, recv3,
           field_sem, load_sem, small_sem, halo_send, halo_recv,
           pick_send, pick_recv, s1_send, s1_recv, s2_send, s2_recv, s3_send, s3_recv):
    rows, width = fbuf.shape
    half = width // 2
    bs = raw_main.shape[2]
    kc = 6
    nb = rows // bs
    groups = nb // GROUP
    ops = (ops0, ops1, ops2, ops3)
    re_bufs, im_bufs, ni_bufs = (re0, re1), (im0, im1), (ni0, ni1)
    me_d = lax.axis_index("depth")
    me_f = lax.axis_index("freq")
    first_row = me_d * rows
    core = lax.rem(me_f, 2)
    z = lax.rem(me_f // 2, NZH)
    y = lax.rem(me_f // (2 * NZH), NY)
    x = me_f // (2 * NZH * NY)
    sibling = me_f + 1 - 2 * core

    def chip_of(ox, oy, oz):
        return (lax.rem(x + ox, NX) * NY + lax.rem(y + oy, NY)) * NZH + lax.rem(z + oz, NZH)

    def device_of(ox, oy, oz, oc=0):
        return {"freq": chip_of(ox, oy, oz) * 2 + lax.rem(core + oc, 2)}

    fch = fbuf.shape[0] // groups

    def field_copy(g):
        at = pl.ds(pl.multiple_of(g * fch, fch), fch)
        return pltpu.make_async_copy(field_hbm.at[at], fbuf.at[at], field_sem.at[g])

    def ops_copies(g):
        at = pl.ds(g * GROUP, GROUP)
        return [pltpu.make_async_copy(src.at[at], dst.at[at], load_sem.at[which, g])
                for which, (src, dst) in enumerate(((main_hbm, raw_main), (side_hbm, raw_side)))]

    small = [pltpu.make_async_copy(src, dst, small_sem.at[i]) for i, (src, dst) in enumerate(
        ((coupling_hbm, coupling), (floors_hbm, floors), (freqs_hbm, freqs),
         (receivers_hbm, receivers)))]
    field_copy(0).start()
    field_copy(groups - 1).start()
    small[0].start()
    small[1].start()
    for copy in ops_copies(0):
        copy.start(priority=1)
    field_copy(1).start()

    def start_group(g, carry):
        field_copy(g + 1).start()
        for copy in ops_copies(g):
            copy.start(priority=1)
        return carry
    lax.fori_loop(1, groups - 2, start_group, 0)
    for g in (groups - 2, groups - 1):
        for copy in ops_copies(g):
            copy.start(priority=1)
    small[2].start()
    small[3].start()

    barrier = pltpu.get_barrier_semaphore()
    greeted = 0
    peers = [{"depth": 1 - me_d, "freq": me_f}, {"depth": 1 - me_d, "freq": sibling}]
    peers += [{"freq": sibling}, device_of(0, 0, 1), device_of(0, 0, 1, 1)]
    peers += [device_of(o, 0, 0) for o in range(1, NX)] + [device_of(0, o, 0) for o in range(1, NY)]
    for peer in peers:
        pl.semaphore_signal(barrier, inc=1, device_id=peer, device_id_type=MESH)
        greeted += 1

    for buf in (final_re, final_im):
        buf[rows:, :] = jnp.zeros((buf.shape[0] - rows, half), F32)

    from_col = lax.broadcasted_iota(jnp.int32, (width, width), 0)
    to_col = lax.broadcasted_iota(jnp.int32, (width, width), 1)
    wanted = jnp.where(to_col < half, 2 * to_col, 2 * (to_col - half) + 1)
    order_buf[...] = jnp.where(from_col == wanted, 1.0, 0.0).astype(BF16)

    def put_w(parity, b, re, im):
        at = pl.ds(pl.multiple_of((b + 1) * bs, bs), bs)
        re_bufs[parity][at, :] = re
        im_bufs[parity][at, :] = im
        ni_bufs[parity][at, :] = -im

    zero_edge = jnp.zeros((bs, half), BF16)
    for buf in (re0, re1, im0, im1, ni0, ni1):
        buf[:bs, :] = zero_edge
        buf[(nb + 1) * bs:, :] = zero_edge

    def enter(g):
        at = pl.ds(pl.multiple_of(g * fch, fch), fch)
        got = jnp.dot(fbuf[at, :], order_buf[...], preferred_element_type=F32).astype(BF16)
        for i in range(GROUP):
            one = got[i * bs:(i + 1) * bs, :]
            put_w(0, g * GROUP + i, one[:, :half], one[:, half:])

    field_copy(0).wait()
    field_copy(groups - 1).wait()
    small[0].wait()
    small[1].wait()
    enter(0)
    enter(groups - 1)
    c16 = jnp.broadcast_to(coupling[...], (16, width))
    high = c16.astype(BF16)
    rest = c16 - high.astype(F32)
    mid = rest.astype(BF16)
    low = (rest - mid.astype(F32)).astype(BF16)
    three = jnp.dot(jnp.concatenate([high, mid, low], axis=0), order_buf[...],
                    preferred_element_type=F32)
    weights[...] = (three[:8] + three[16:24]) + three[32:40]

    below = 1 - me_d
    edge = pl.ds(pl.multiple_of((below * (nb - 1) + 1) * bs, bs), bs)

    def halo_copies(step):
        return [pltpu.make_async_remote_copy(
            src_ref=bufs[step % 2].at[edge],
            dst_ref=halo.at[step, which],
            send_sem=halo_send.at[step, which],
            recv_sem=halo_recv.at[step, which],
            device_id={"depth": 1 - me_d},
            device_id_type=MESH,
        ) for which, bufs in enumerate((re_bufs, im_bufs))]

    def halo_start(step):
        for copy in halo_copies(step):
            copy.start()

    def halo_wait(step):
        for copy in halo_copies(step):
            copy.wait()

    def halo_put(step):
        put_w(step % 2, below * (nb + 1) - 1, halo[step, 0], halo[step, 1])

    row_iota = lax.broadcasted_iota(jnp.int32, (bs, half), 0)

    def piece_of(step, g, i, p):
        if step > 0:
            return ops[i][g, p]
        pair = [raw.at[g * GROUP + i][pl.ds(p, bs, stride=kc), :] for raw in (raw_main, raw_side)]
        piece = jnp.concatenate(pair, axis=0)
        ops[i][g, p] = piece
        return piece

    def multiply(step, g, i):
        b = g * GROUP + i
        parity = step % 2
        acc = None
        for k in range(3):
            at = pl.ds(pl.multiple_of((b + k) * bs, bs), bs)
            re, im, ni = re_bufs[parity][at, :], im_bufs[parity][at, :], ni_bufs[parity][at, :]
            near = jnp.concatenate([jnp.concatenate([re, im], axis=1),
                                    jnp.concatenate([ni, re], axis=1)], axis=0)
            block = jnp.concatenate(
                [piece_of(step, g, i, 2 * k), piece_of(step, g, i, 2 * k + 1)], axis=1)
            part = jnp.dot(block, near, preferred_element_type=F32)
            acc = part if acc is None else acc + part
        m, c = acc[:bs], acc[bs:]
        wr = weights[0:1, :half]
        wi = weights[0:1, half:]
        re = m[:, :half] + wr * c[:, :half] - wi * c[:, half:]
        im = m[:, half:] + wr * c[:, half:] + wi * c[:, :half]
        damp = jnp.where(row_iota >= floors[step] - (first_row + b * bs), F32(0.5), F32(1.0))
        re = damp * re
        im = damp * im
        if step == STEPS - 1:
            at = pl.ds(pl.multiple_of(b * bs, bs), bs)
            final_re[at, :] = re
            final_im[at, :] = im
        else:
            put_w(1 - parity, b, re.astype(BF16), im.astype(BF16))

    def first_step(g, skip=0, last_field=None):
        for copy in ops_copies(g):
            copy.wait()
        if last_field is None:
            field_copy(g + 2).wait()
        for i in range(GROUP):
            if i >= skip:
                multiply(0, g, i)
        if last_field is None:
            enter(g + 2)

    field_copy(1).wait()
    enter(1)
    pl.semaphore_wait(barrier, greeted)
    halo_start(0)
    first_step(0, skip=1)

    def first_loop(g, carry):
        first_step(g)
        return carry

    lax.fori_loop(1, groups - 3, first_loop, 0)
    first_step(groups - 3, last_field=False)
    first_step(groups - 2, last_field=False)
    for copy in ops_copies(groups - 1):
        copy.wait()
    halo_wait(0)
    for i in range(GROUP - 1):
        multiply(0, groups - 1, i)
    halo_put(0)
    multiply(0, 0, 0)
    multiply(0, groups - 1, GROUP - 1)
    small[2].wait()
    small[3].wait()
    spot = receivers[...] - first_row
    inside = jnp.logical_and(spot >= 0, spot < rows)
    near_rows[...] = jnp.where(inside, spot, rows)
    spot_copies = [
        pltpu.make_async_copy(near_rows.at[j], spots.at[pl.ds(j * bs, bs)], small_sem.at[4 + j])
        for j in range(near_rows.shape[0])]
    for copy in spot_copies:
        copy.start()

    for step in range(1, STEPS):
        halo_start(step)
        for b in range(1, nb - 1 - LATE):
            multiply(step, b // GROUP, b % GROUP)
        halo_wait(step)
        for b in range(nb - 1 - LATE, nb - 1):
            multiply(step, b // GROUP, b % GROUP)
        halo_put(step)
        multiply(step, 0, 0)
        multiply(step, groups - 1, GROUP - 1)

    here = 2 * bs

    def pick(owner, side):
        base = owner * here + lax.rem(core + side, 2) * bs

        def take(q, carry):
            for j in range(16):
                row = q * 16 + j
                spot = spots[base + row]
                grab_re[pl.ds(row, 1), :] = final_re[pl.ds(spot, 1), :]
                grab_im[pl.ds(row, 1), :] = final_im[pl.ds(spot, 1), :]
            return carry

        lax.fori_loop(0, bs // 16, take, 0, unroll=2)
        return jnp.concatenate([grab_re[...], grab_im[...]], axis=1).astype(BF16)

    for copy in spot_copies:
        copy.wait()

    def move(src, dst, sems, at, to):
        return pltpu.make_async_remote_copy(
            src_ref=src, dst_ref=dst, send_sem=sems[0].at[at], recv_sem=sems[1].at[at],
            device_id=to, device_id_type=MESH)

    pick_sems = (pick_send, pick_recv)
    across = []
    for side, line in enumerate((me_f, sibling)):
        across.append(move(picked.at[side], pick_in.at[side], pick_sems, side,
                           {"depth": 1 - me_d, "freq": line}))
    beside = move(own.at[1], sib_own, pick_sems, 2, {"freq": sibling})
    for side in range(2):
        picked[side] = pick(1 - me_d, side)
        across[side].start()
    own[1] = pick(me_d, 1)
    beside.start()
    own[0] = pick(me_d, 0)

    chips = NX * NY * NZH
    times = NT // (2 * chips)
    count = lax.broadcasted_iota(jnp.int32, (chips, half), 0).astype(F32)
    late = lax.broadcasted_iota(jnp.int32, (2 * times, half), 0)
    late = jnp.where(late < times, late + core * times, late - core * times).astype(F32)
    for h, line in enumerate((me_f, sibling)):
        tone = freqs[pl.ds(line, 1), :]
        at = slice(h * half, (h + 1) * half)
        cos, sin = turn((tone * count) * F32(1.0 / chips))
        coarse[0, :, at] = cos
        coarse[1, :, at] = -sin
        cos, sin = turn((tone * late) * F32(1.0 / NT))
        fine[0, :, at] = cos
        fine[1, :, at] = sin
    th = times

    def place_of(off):
        return lax.rem(off, 2) * 2 + off // 2

    def basis_of(q, carry):
        ox, oy = q // NY, lax.rem(q, NY)
        for oz in range(NZH):
            chip = chip_of(ox, oy, oz)
            ca = coarse[0, pl.ds(chip, 1), :]
            na = coarse[1, pl.ds(chip, 1), :]
            for part, (basis, place) in enumerate(
                    ((basis_a, place_of(oy) * NX + ox), (basis_b, place_of(ox) * NY + oy))):
                at = pl.ds(pl.multiple_of((place * NZH + oz) * th, th), th)
                cb = fine[0, part * th:(part + 1) * th, :]
                sb = fine[1, part * th:(part + 1) * th, :]
                cos = (ca * cb + na * sb).astype(BF16)
                nsin = (na * cb - ca * sb).astype(BF16)
                for h in range(2):
                    basis[at, 2 * h * half:(2 * h + 1) * half] = cos[:, h * half:(h + 1) * half]
                    basis[at, (2 * h + 1) * half:(2 * h + 2) * half] = nsin[:, h * half:(h + 1) * half]
        return carry

    lax.fori_loop(0, NX * NY, basis_of, 0, unroll=2)

    for copy in across:
        copy.wait()
    beside.wait()
    for h, one in enumerate((own.at[0], sib_own)):
        owned[:, h * width:(h + 1) * width] = (
            one[...].astype(F32) + pick_in[h].astype(F32)).astype(BF16)

    slab = NY * NZH * th
    piece = NZH * th
    s1, s2, s3 = (s1_send, s1_recv), (s2_send, s2_recv), (s3_send, s3_recv)

    def over(part, off):
        return device_of(off, 0, 0) if part == 0 else device_of(0, off, 0)

    def series(basis, at):
        return lax.dot_general(basis[at, :], owned[...], (((1,), (1,)), ((), ())),
                               preferred_element_type=F32)

    def first_copy(part, off, place):
        return move(send1.at[part, off - 1, place], recv1.at[part, off - 1, place], s1,
                    (part, off - 1, place), over(part, off))

    def second_copy(part, off, late):
        at = pl.ds(0, th) if late else pl.ds(th, piece - th)
        return move(send2.at[part, off - 1, at], recv2.at[part, off - 1, at], s2,
                    (part, off - 1, late), over(1 - part, off))

    third = [move(send3.at[k], recv3.at[k], s3, k, to) for k, to in enumerate(
        (device_of(0, 0, 1), device_of(0, 0, 1, 1), {"freq": sibling}))]

    for places in ((1,), (2, 3), (0,)):
        size = NX * piece
        for part, basis in enumerate((basis_a, basis_b)):
            got = series(basis, slice(places[0] * size, (places[-1] + 1) * size))
            for k, place in enumerate(places):
                keep[part, place] = got[k * size:k * size + piece]
                for off in range(1, NX):
                    send1[part, off - 1, place] = got[
                        k * size + off * piece:k * size + (off + 1) * piece].astype(BF16)
        for place in places:
            for off in (2, 1, 3):
                for part in range(2):
                    first_copy(part, off, place).start()

    def total_of(recv, count, part, place, first, size):
        at = slice(first, first + size)
        total = keep[part, place, at, :]
        for k in range(count):
            one = recv[part, k, place, at, :] if recv is recv1 else recv[part, k, at, :]
            total = total + one.astype(F32)
        return total

    for place, off2 in ((1, 2), (2, 1), (3, 3)):
        for part in range(2):
            for off in range(1, NX):
                first_copy(part, off, place).wait()
            send2[part, off2 - 1] = total_of(recv1, NX - 1, part, place, 0, piece).astype(BF16)
            for late in range(2):
                second_copy(part, off2, late).start()
    for part in range(2):
        for off in range(1, NX):
            first_copy(part, off, 0).wait()
        keep[part, 0] = total_of(recv1, NX - 1, part, 0, 0, piece)
    for part in range(2):
        for off in range(1, NY):
            second_copy(part, off, 0).wait()
        send3[part] = total_of(recv2, NY - 1, part, 0, th, th).astype(BF16)
        third[part].start()
    for part in (1, 0):
        for off in range(1, NY):
            second_copy(part, off, 1).wait()
        total = total_of(recv2, NY - 1, part, 0, 0, th)
        if part:
            send3[2] = total.astype(BF16)
            third[2].start()
        else:
            keep[0, 0, :th, :] = total
    for copy in third:
        copy.wait()
    mine = (keep[0, 0, :th, :] + recv3[0].astype(F32)) * factor
    theirs = (recv3[1].astype(F32) + recv3[2].astype(F32)) * factor
    first = core == 0
    out[:, :bs] = jnp.where(first, mine, theirs)
    out[:, bs:] = jnp.where(first, theirs, mine)


def local(depth_n, freq_n, pressure_field, block_main, block_coupled, coupling, frequencies,
          receivers, floors):
    rows, width = pressure_field.shape
    bs = block_main.shape[3]
    half = width // 2
    nb = rows // bs
    here = receivers.shape[0] // depth_n
    times = NT // freq_n
    factor = 1.0 / math.sqrt(frequencies.shape[0])
    vmem = pl.BlockSpec(memory_space=pltpu.VMEM)
    hbm = pl.BlockSpec(memory_space=pl.ANY)
    chips = NX * NY * NZH
    th = times
    slab = NY * NZH * th
    dma = pltpu.SemaphoreType.DMA
    result = pl.pallas_call(
        functools.partial(kernel, depth_n, factor),
        out_shape=jax.ShapeDtypeStruct((times, here), F32),
        in_specs=[hbm] * 7,
        out_specs=vmem,
        scratch_shapes=[
            pltpu.VMEM((rows, width), BF16),
            pltpu.VMEM((nb, 6 * bs, bs), BF16),
            pltpu.VMEM((nb, 6 * bs, bs), BF16),
            *[pltpu.VMEM((nb // GROUP, 6, 2 * bs, bs), BF16) for _ in range(GROUP)],
            *[pltpu.VMEM(((nb + 2) * bs, half), BF16) for _ in range(6)],
            pltpu.VMEM((rows + 8, half), F32),
            pltpu.VMEM((rows + 8, half), F32),
            pltpu.VMEM((STEPS, 2, bs, half), BF16),
            pltpu.VMEM((width, width), BF16),
            pltpu.VMEM((1, width), F32),
            pltpu.VMEM((frequencies.shape[0] // half, half), F32),
            pltpu.VMEM((receivers.shape[0] // bs, bs), jnp.int32),
            pltpu.SMEM((STEPS,), jnp.int32),
            pltpu.VMEM((8, width), F32),
            pltpu.VMEM((receivers.shape[0] // bs, bs), jnp.int32),
            pltpu.SMEM((receivers.shape[0],), jnp.int32),
            pltpu.VMEM((bs, half), F32),
            pltpu.VMEM((bs, half), F32),
            pltpu.VMEM((2, bs, width), BF16),
            pltpu.VMEM((2, bs, width), BF16),
            pltpu.VMEM((2, bs, width), BF16),
            pltpu.VMEM((bs, width), BF16),
            pltpu.VMEM((bs, 2 * width), BF16),
            pltpu.VMEM((2, chips, width), F32),
            pltpu.VMEM((2, 2 * times, width), F32),
            pltpu.VMEM((NX * slab, 2 * width), BF16),
            pltpu.VMEM((NX * slab, 2 * width), BF16),
            pltpu.VMEM((2, NY, NZH * th, bs), F32),
            pltpu.VMEM((2, NX - 1, NY, NZH * th, bs), BF16),
            pltpu.VMEM((2, NX - 1, NY, NZH * th, bs), BF16),
            pltpu.VMEM((2, NY - 1, NZH * th, bs), BF16),
            pltpu.VMEM((2, NY - 1, NZH * th, bs), BF16),
            pltpu.VMEM((3, th, bs), BF16),
            pltpu.VMEM((3, th, bs), BF16),
            dma((nb // GROUP,)),
            dma((2, nb // GROUP)),
            dma((4 + receivers.shape[0] // bs,)),
            dma((STEPS, 2)),
            dma((STEPS, 2)),
            dma((3,)),
            dma((3,)),
            dma((2, NX - 1, NY)),
            dma((2, NX - 1, NY)),
            dma((2, NY - 1, 2)),
            dma((2, NY - 1, 2)),
            dma((3,)),
            dma((3,)),
        ],
        compiler_params=pltpu.CompilerParams(
            collective_id=0, has_side_effects=True, vmem_limit_bytes=64 * 1024 * 1024 - 128 * 1024
        ),
    )(
        pressure_field,
        block_main.reshape(nb, 6 * bs, bs),
        block_coupled.reshape(nb, 6 * bs, bs),
        coupling.reshape(1, width),
        frequencies.reshape(-1, half),
        receivers.reshape(-1, bs),
        floors,
    )
    return result.T


def solution(mesh):
    in_specs = (
        P("depth", "freq"),
        P("depth", None, None, None),
        P("depth", None, None, None),
        P("freq"),
        P(),
        P(),
        P(),
    )
    body = functools.partial(local, mesh.shape["depth"], mesh.shape["freq"])
    return jax.shard_map(body, mesh=mesh, in_specs=in_specs, out_specs=P("depth", "freq"),
                         check_vma=False)
```

```python
import functools
import math

import jax
import jax.numpy as jnp
from jax import lax
from jax.experimental import pallas as pl
from jax.experimental.pallas import tpu as pltpu
from jax.sharding import PartitionSpec as P

NT = 2048
STEPS = 4
NX, NY, NZH = 4, 4, 2
GROUP = 4
LATE = 2

COS_TERMS = (1.0, -19.739208221435547, 64.93939208984375, -85.45665740966797,
             60.242130279541016, -26.4046688079834, 7.800131320953369, -1.453112244606018)
SIN_TERMS = (6.2831854820251465, -41.34170150756836, 81.6052474975586, -76.70580291748047,
             42.05775451660156, -15.086565017700195, 3.7813189029693604, -0.6207787394523621)

MESH = pl.DeviceIdType.MESH
F32 = jnp.float32
BF16 = jnp.bfloat16


def poly(terms, z):
    total = jnp.full_like(z, terms[-1])
    for term in terms[-2::-1]:
        total = total * z + F32(term)
    return total


def turn(y):
    p = y - jnp.floor(y)
    r = jnp.where(p > 0.5, p - 1.0, p)
    z = r * r
    return poly(COS_TERMS, z), r * poly(SIN_TERMS, z)


def kernel(depth_n, factor,
           field_hbm, main_hbm, side_hbm, coupling_hbm, freqs_hbm, receivers_hbm, floors_hbm, out,
           fbuf, raw_main, raw_side,
           ops0, ops1, ops2, ops3, re0, re1, im0, im1, ni0, ni1,
           final_re, final_im, halo, order_buf,
           coupling, freqs, receivers, floors, weights, near_rows, spots, grab_re, grab_im,
           picked, own, pick_in, sib_own, owned,
           coarse, fine, basis_a, basis_b, keep, send1, recv1, send2, recv2,
           field_sem, load_sem, small_sem, halo_send, halo_recv,
           pick_send, pick_recv, s1_send, s1_recv, s2_send, s2_recv):
    rows, width = fbuf.shape
    half = width // 2
    bs = raw_main.shape[2]
    kc = 6
    nb = rows // bs
    groups = nb // GROUP
    ops = (ops0, ops1, ops2, ops3)
    re_bufs, im_bufs, ni_bufs = (re0, re1), (im0, im1), (ni0, ni1)
    me_d = lax.axis_index("depth")
    me_f = lax.axis_index("freq")
    first_row = me_d * rows
    core = lax.rem(me_f, 2)
    z = lax.rem(me_f // 2, NZH)
    y = lax.rem(me_f // (2 * NZH), NY)
    x = me_f // (2 * NZH * NY)
    sibling = me_f + 1 - 2 * core

    def chip_of(ox, oy, oz):
        return (lax.rem(x + ox, NX) * NY + lax.rem(y + oy, NY)) * NZH + lax.rem(z + oz, NZH)

    def device_of(ox, oy, oz, oc=0):
        return {"freq": chip_of(ox, oy, oz) * 2 + lax.rem(core + oc, 2)}

    fch = fbuf.shape[0] // groups

    def field_copy(g):
        at = pl.ds(pl.multiple_of(g * fch, fch), fch)
        return pltpu.make_async_copy(field_hbm.at[at], fbuf.at[at], field_sem.at[g])

    def ops_copies(g):
        at = pl.ds(g * GROUP, GROUP)
        return [pltpu.make_async_copy(src.at[at], dst.at[at], load_sem.at[which, g])
                for which, (src, dst) in enumerate(((main_hbm, raw_main), (side_hbm, raw_side)))]

    small = [pltpu.make_async_copy(src, dst, small_sem.at[i]) for i, (src, dst) in enumerate(
        ((coupling_hbm, coupling), (floors_hbm, floors), (freqs_hbm, freqs),
         (receivers_hbm, receivers)))]
    field_copy(0).start()
    field_copy(groups - 1).start()
    small[0].start()
    small[1].start()
    for copy in ops_copies(0):
        copy.start(priority=1)
    field_copy(1).start()

    def start_group(g, carry):
        field_copy(g + 1).start()
        for copy in ops_copies(g):
            copy.start(priority=1)
        return carry
    lax.fori_loop(1, groups - 2, start_group, 0)
    for g in (groups - 2, groups - 1):
        for copy in ops_copies(g):
            copy.start(priority=1)
    small[2].start()
    small[3].start()

    barrier = pltpu.get_barrier_semaphore()
    greeted = 0
    peers = [{"depth": 1 - me_d, "freq": me_f}, {"depth": 1 - me_d, "freq": sibling}]
    peers += [device_of(o, 0, 0) for o in range(1, NX)]
    peers += [device_of(0, o, oz) for o in range(NY) for oz in range(NZH) if o or oz]
    peers += [device_of(o, 0, oz, 1) for o in range(NX) for oz in range(NZH)]
    for peer in peers:
        pl.semaphore_signal(barrier, inc=1, device_id=peer, device_id_type=MESH)
        greeted += 1

    for buf in (final_re, final_im):
        buf[rows:, :] = jnp.zeros((buf.shape[0] - rows, half), F32)

    from_col = lax.broadcasted_iota(jnp.int32, (width, width), 0)
    to_col = lax.broadcasted_iota(jnp.int32, (width, width), 1)
    wanted = jnp.where(to_col < half, 2 * to_col, 2 * (to_col - half) + 1)
    order_buf[...] = jnp.where(from_col == wanted, 1.0, 0.0).astype(BF16)

    def put_w(parity, b, re, im):
        at = pl.ds(pl.multiple_of((b + 1) * bs, bs), bs)
        re_bufs[parity][at, :] = re
        im_bufs[parity][at, :] = im
        ni_bufs[parity][at, :] = -im

    zero_edge = jnp.zeros((bs, half), BF16)
    for buf in (re0, re1, im0, im1, ni0, ni1):
        buf[:bs, :] = zero_edge
        buf[(nb + 1) * bs:, :] = zero_edge

    def enter(g):
        at = pl.ds(pl.multiple_of(g * fch, fch), fch)
        got = jnp.dot(fbuf[at, :], order_buf[...], preferred_element_type=F32).astype(BF16)
        for i in range(GROUP):
            one = got[i * bs:(i + 1) * bs, :]
            put_w(0, g * GROUP + i, one[:, :half], one[:, half:])

    field_copy(0).wait()
    field_copy(groups - 1).wait()
    small[0].wait()
    small[1].wait()
    enter(0)
    enter(groups - 1)
    c16 = jnp.broadcast_to(coupling[...], (16, width))
    high = c16.astype(BF16)
    rest = c16 - high.astype(F32)
    mid = rest.astype(BF16)
    low = (rest - mid.astype(F32)).astype(BF16)
    three = jnp.dot(jnp.concatenate([high, mid, low], axis=0), order_buf[...],
                    preferred_element_type=F32)
    weights[...] = (three[:8] + three[16:24]) + three[32:40]

    below = 1 - me_d
    edge = pl.ds(pl.multiple_of((below * (nb - 1) + 1) * bs, bs), bs)

    def halo_copies(step):
        return [pltpu.make_async_remote_copy(
            src_ref=bufs[step % 2].at[edge],
            dst_ref=halo.at[step, which],
            send_sem=halo_send.at[step, which],
            recv_sem=halo_recv.at[step, which],
            device_id={"depth": 1 - me_d},
            device_id_type=MESH,
        ) for which, bufs in enumerate((re_bufs, im_bufs))]

    def halo_start(step):
        for copy in halo_copies(step):
            copy.start()

    def halo_wait(step):
        for copy in halo_copies(step):
            copy.wait()

    def halo_put(step):
        put_w(step % 2, below * (nb + 1) - 1, halo[step, 0], halo[step, 1])

    row_iota = lax.broadcasted_iota(jnp.int32, (bs, half), 0)

    def piece_of(step, g, i, p):
        if step > 0:
            return ops[i][g, p]
        pair = [raw.at[g * GROUP + i][pl.ds(p, bs, stride=kc), :] for raw in (raw_main, raw_side)]
        piece = jnp.concatenate(pair, axis=0)
        ops[i][g, p] = piece
        return piece

    def multiply(step, g, i):
        b = g * GROUP + i
        parity = step % 2
        acc = None
        for k in range(3):
            at = pl.ds(pl.multiple_of((b + k) * bs, bs), bs)
            re, im, ni = re_bufs[parity][at, :], im_bufs[parity][at, :], ni_bufs[parity][at, :]
            near = jnp.concatenate([jnp.concatenate([re, im], axis=1),
                                    jnp.concatenate([ni, re], axis=1)], axis=0)
            block = jnp.concatenate(
                [piece_of(step, g, i, 2 * k), piece_of(step, g, i, 2 * k + 1)], axis=1)
            part = jnp.dot(block, near, preferred_element_type=F32)
            acc = part if acc is None else acc + part
        m, c = acc[:bs], acc[bs:]
        wr = weights[0:1, :half]
        wi = weights[0:1, half:]
        re = m[:, :half] + wr * c[:, :half] - wi * c[:, half:]
        im = m[:, half:] + wr * c[:, half:] + wi * c[:, :half]
        damp = jnp.where(row_iota >= floors[step] - (first_row + b * bs), F32(0.5), F32(1.0))
        re = damp * re
        im = damp * im
        if step == STEPS - 1:
            at = pl.ds(pl.multiple_of(b * bs, bs), bs)
            final_re[at, :] = re
            final_im[at, :] = im
        else:
            put_w(1 - parity, b, re.astype(BF16), im.astype(BF16))

    def first_step(g, skip=0, last_field=None):
        for copy in ops_copies(g):
            copy.wait()
        if last_field is None:
            field_copy(g + 2).wait()
        for i in range(GROUP):
            if i >= skip:
                multiply(0, g, i)
        if last_field is None:
            enter(g + 2)

    field_copy(1).wait()
    enter(1)
    pl.semaphore_wait(barrier, greeted)
    halo_start(0)
    first_step(0, skip=1)

    def first_loop(g, carry):
        first_step(g)
        return carry

    lax.fori_loop(1, groups - 3, first_loop, 0)
    first_step(groups - 3, last_field=False)
    first_step(groups - 2, last_field=False)
    for copy in ops_copies(groups - 1):
        copy.wait()
    halo_wait(0)
    for i in range(GROUP - 1):
        multiply(0, groups - 1, i)
    halo_put(0)
    multiply(0, 0, 0)
    multiply(0, groups - 1, GROUP - 1)
    small[2].wait()
    small[3].wait()
    spot = receivers[...] - first_row
    inside = jnp.logical_and(spot >= 0, spot < rows)
    near_rows[...] = jnp.where(inside, spot, rows)
    spot_copies = [
        pltpu.make_async_copy(near_rows.at[j], spots.at[pl.ds(j * bs, bs)], small_sem.at[4 + j])
        for j in range(near_rows.shape[0])]
    for copy in spot_copies:
        copy.start()

    for step in range(1, STEPS):
        halo_start(step)
        for b in range(1, nb - 1 - LATE):
            multiply(step, b // GROUP, b % GROUP)
        halo_wait(step)
        for b in range(nb - 1 - LATE, nb - 1):
            multiply(step, b // GROUP, b % GROUP)
        halo_put(step)
        multiply(step, 0, 0)
        multiply(step, groups - 1, GROUP - 1)

    here = 2 * bs

    def pick(owner, side):
        base = owner * here + lax.rem(core + side, 2) * bs

        def take(q, carry):
            for j in range(16):
                row = q * 16 + j
                spot = spots[base + row]
                grab_re[pl.ds(row, 1), :] = final_re[pl.ds(spot, 1), :]
                grab_im[pl.ds(row, 1), :] = final_im[pl.ds(spot, 1), :]
            return carry

        lax.fori_loop(0, bs // 16, take, 0, unroll=2)
        return jnp.concatenate([grab_re[...], grab_im[...]], axis=1).astype(BF16)

    for copy in spot_copies:
        copy.wait()

    def move(src, dst, sems, at, to):
        return pltpu.make_async_remote_copy(
            src_ref=src, dst_ref=dst, send_sem=sems[0].at[at], recv_sem=sems[1].at[at],
            device_id=to, device_id_type=MESH)

    pick_sems = (pick_send, pick_recv)
    across = []
    for side, line in enumerate((me_f, sibling)):
        across.append(move(picked.at[side], pick_in.at[side], pick_sems, side,
                           {"depth": 1 - me_d, "freq": line}))
    beside = move(own.at[1], sib_own, pick_sems, 2, {"freq": sibling})
    for side in range(2):
        picked[side] = pick(1 - me_d, side)
        across[side].start()
    own[1] = pick(me_d, 1)
    beside.start()
    own[0] = pick(me_d, 0)

    chips = NX * NY * NZH
    times = NT // (2 * chips)
    count = lax.broadcasted_iota(jnp.int32, (chips, half), 0).astype(F32)
    late = lax.broadcasted_iota(jnp.int32, (2 * times, half), 0)
    late = jnp.where(late < times, late + core * times, late - core * times).astype(F32)
    for h, line in enumerate((me_f, sibling)):
        tone = freqs[pl.ds(line, 1), :]
        at = slice(h * half, (h + 1) * half)
        cos, sin = turn((tone * count) * F32(1.0 / chips))
        coarse[0, :, at] = cos
        coarse[1, :, at] = -sin
        cos, sin = turn((tone * late) * F32(1.0 / NT))
        fine[0, :, at] = cos
        fine[1, :, at] = sin
    th = times

    def place_of(off):
        return lax.rem(off, 2) * 2 + off // 2

    def basis_of(q, carry):
        ox, oy = q // NY, lax.rem(q, NY)
        for oz in range(NZH):
            chip = chip_of(ox, oy, oz)
            ca = coarse[0, pl.ds(chip, 1), :]
            na = coarse[1, pl.ds(chip, 1), :]
            for part, (basis, place) in enumerate(
                    ((basis_a, place_of(oy) * NX + ox), (basis_b, place_of(ox) * NY + oy))):
                at = pl.ds(pl.multiple_of((place * NZH + oz) * th, th), th)
                cb = fine[0, part * th:(part + 1) * th, :]
                sb = fine[1, part * th:(part + 1) * th, :]
                cos = (ca * cb + na * sb).astype(BF16)
                nsin = (na * cb - ca * sb).astype(BF16)
                for h in range(2):
                    basis[at, 2 * h * half:(2 * h + 1) * half] = cos[:, h * half:(h + 1) * half]
                    basis[at, (2 * h + 1) * half:(2 * h + 2) * half] = nsin[:, h * half:(h + 1) * half]
        return carry

    lax.fori_loop(0, NX * NY, basis_of, 0, unroll=2)

    for copy in across:
        copy.wait()
    beside.wait()
    for h, one in enumerate((own.at[0], sib_own)):
        owned[:, h * width:(h + 1) * width] = (
            one[...].astype(F32) + pick_in[h].astype(F32)).astype(BF16)

    slab = NY * NZH * th
    piece = NZH * th
    s1, s2 = (s1_send, s1_recv), (s2_send, s2_recv)

    def over(part, off):
        return device_of(off, 0, 0) if part == 0 else device_of(0, off, 0)

    def series(basis, at):
        return lax.dot_general(basis[at, :], owned[...], (((1,), (1,)), ((), ())),
                               preferred_element_type=F32)

    def first_copy(part, off, place):
        return move(send1.at[part, off - 1, place], recv1.at[part, off - 1, place], s1,
                    (part, off - 1, place), over(part, off))

    def second_copy(part, place, oz):
        off = (place % 2) * 2 + place // 2
        to = device_of(off, 0, oz, 1) if part else device_of(0, off, oz)
        return move(send2.at[part, place, oz], recv2.at[part, place, oz], s2,
                    (part, place, oz), to)

    for places in ((1,), (2, 3), (0,)):
        size = NX * piece
        for part, basis in enumerate((basis_a, basis_b)):
            got = series(basis, slice(places[0] * size, (places[-1] + 1) * size))
            for k, place in enumerate(places):
                keep[part, place] = got[k * size:k * size + piece]
                for off in range(1, NX):
                    send1[part, off - 1, place] = got[
                        k * size + off * piece:k * size + (off + 1) * piece].astype(BF16)
        for place in places:
            for off in (2, 1, 3):
                for part in range(2):
                    first_copy(part, off, place).start()

    for place in (1, 2, 3, 0):
        for part in range(2):
            for off in range(1, NX):
                first_copy(part, off, place).wait()
            total = keep[part, place]
            for k in range(NX - 1):
                total = total + recv1[part, k, place].astype(F32)
            for oz in (1, 0):
                one = total[oz * th:(oz + 1) * th]
                if part or place or oz:
                    send2[part, place, oz] = one.astype(BF16)
                    second_copy(part, place, oz).start()
                else:
                    keep[0, 0, :th, :] = one
    came = [(part, place, oz) for part in range(2) for place in range(NY) for oz in range(NZH)
            if part or place or oz]
    for at in came:
        second_copy(*at).wait()
    both = [keep[0, 0, :th, :], None]
    for part, place, oz in came:
        one = recv2[part, place, oz].astype(F32)
        both[part] = one if both[part] is None else both[part] + one
    mine, theirs = both[0] * factor, both[1] * factor
    first = core == 0
    out[:, :bs] = jnp.where(first, mine, theirs)
    out[:, bs:] = jnp.where(first, theirs, mine)


def local(depth_n, freq_n, pressure_field, block_main, block_coupled, coupling, frequencies,
          receivers, floors):
    rows, width = pressure_field.shape
    bs = block_main.shape[3]
    half = width // 2
    nb = rows // bs
    here = receivers.shape[0] // depth_n
    times = NT // freq_n
    factor = 1.0 / math.sqrt(frequencies.shape[0])
    vmem = pl.BlockSpec(memory_space=pltpu.VMEM)
    hbm = pl.BlockSpec(memory_space=pl.ANY)
    chips = NX * NY * NZH
    th = times
    slab = NY * NZH * th
    dma = pltpu.SemaphoreType.DMA
    result = pl.pallas_call(
        functools.partial(kernel, depth_n, factor),
        out_shape=jax.ShapeDtypeStruct((times, here), F32),
        in_specs=[hbm] * 7,
        out_specs=vmem,
        scratch_shapes=[
            pltpu.VMEM((rows, width), BF16),
            pltpu.VMEM((nb, 6 * bs, bs), BF16),
            pltpu.VMEM((nb, 6 * bs, bs), BF16),
            *[pltpu.VMEM((nb // GROUP, 6, 2 * bs, bs), BF16) for _ in range(GROUP)],
            *[pltpu.VMEM(((nb + 2) * bs, half), BF16) for _ in range(6)],
            pltpu.VMEM((rows + 8, half), F32),
            pltpu.VMEM((rows + 8, half), F32),
            pltpu.VMEM((STEPS, 2, bs, half), BF16),
            pltpu.VMEM((width, width), BF16),
            pltpu.VMEM((1, width), F32),
            pltpu.VMEM((frequencies.shape[0] // half, half), F32),
            pltpu.VMEM((receivers.shape[0] // bs, bs), jnp.int32),
            pltpu.SMEM((STEPS,), jnp.int32),
            pltpu.VMEM((8, width), F32),
            pltpu.VMEM((receivers.shape[0] // bs, bs), jnp.int32),
            pltpu.SMEM((receivers.shape[0],), jnp.int32),
            pltpu.VMEM((bs, half), F32),
            pltpu.VMEM((bs, half), F32),
            pltpu.VMEM((2, bs, width), BF16),
            pltpu.VMEM((2, bs, width), BF16),
            pltpu.VMEM((2, bs, width), BF16),
            pltpu.VMEM((bs, width), BF16),
            pltpu.VMEM((bs, 2 * width), BF16),
            pltpu.VMEM((2, chips, width), F32),
            pltpu.VMEM((2, 2 * times, width), F32),
            pltpu.VMEM((NX * slab, 2 * width), BF16),
            pltpu.VMEM((NX * slab, 2 * width), BF16),
            pltpu.VMEM((2, NY, NZH * th, bs), F32),
            pltpu.VMEM((2, NX - 1, NY, NZH * th, bs), BF16),
            pltpu.VMEM((2, NX - 1, NY, NZH * th, bs), BF16),
            pltpu.VMEM((2, NY, NZH, th, bs), BF16),
            pltpu.VMEM((2, NY, NZH, th, bs), BF16),
            dma((nb // GROUP,)),
            dma((2, nb // GROUP)),
            dma((4 + receivers.shape[0] // bs,)),
            dma((STEPS, 2)),
            dma((STEPS, 2)),
            dma((3,)),
            dma((3,)),
            dma((2, NX - 1, NY)),
            dma((2, NX - 1, NY)),
            dma((2, NY, NZH)),
            dma((2, NY, NZH)),
        ],
        compiler_params=pltpu.CompilerParams(
            collective_id=0, has_side_effects=True, vmem_limit_bytes=64 * 1024 * 1024 - 128 * 1024
        ),
    )(
        pressure_field,
        block_main.reshape(nb, 6 * bs, bs),
        block_coupled.reshape(nb, 6 * bs, bs),
        coupling.reshape(1, width),
        frequencies.reshape(-1, half),
        receivers.reshape(-1, bs),
        floors,
    )
    return result.T


def solution(mesh):
    in_specs = (
        P("depth", "freq"),
        P("depth", None, None, None),
        P("depth", None, None, None),
        P("freq"),
        P(),
        P(),
        P(),
    )
    body = functools.partial(local, mesh.shape["depth"], mesh.shape["freq"])
    return jax.shard_map(body, mesh=mesh, in_specs=in_specs, out_specs=P("depth", "freq"),
                         check_vma=False)
```

```python
import functools
import math

import jax
import jax.numpy as jnp
from jax import lax
from jax.experimental import pallas as pl
from jax.experimental.pallas import tpu as pltpu
from jax.sharding import PartitionSpec as P

NT = 2048
STEPS = 4
NX, NY, NZH = 4, 4, 2
GROUP = 4
LATE = 2

COS_TERMS = (1.0, -19.739208221435547, 64.93939208984375, -85.45665740966797,
             60.242130279541016, -26.4046688079834, 7.800131320953369, -1.453112244606018)
SIN_TERMS = (6.2831854820251465, -41.34170150756836, 81.6052474975586, -76.70580291748047,
             42.05775451660156, -15.086565017700195, 3.7813189029693604, -0.6207787394523621)

MESH = pl.DeviceIdType.MESH
F32 = jnp.float32
BF16 = jnp.bfloat16


def poly(terms, z):
    total = jnp.full_like(z, terms[-1])
    for term in terms[-2::-1]:
        total = total * z + F32(term)
    return total


def turn(y):
    p = y - jnp.floor(y)
    r = jnp.where(p > 0.5, p - 1.0, p)
    z = r * r
    return poly(COS_TERMS, z), r * poly(SIN_TERMS, z)


def kernel(depth_n, factor,
           field_hbm, main_hbm, side_hbm, coupling_hbm, freqs_hbm, receivers_hbm, floors_hbm, out,
           fbuf, raw_main, raw_side,
           ops0, ops1, ops2, ops3, re0, re1, im0, im1, ni0, ni1,
           final_re, final_im, halo, order_buf,
           coupling, freqs, receivers, floors, weights, near_rows, spots, grab_re, grab_im,
           picked, own, pick_in, sib_own, owned,
           coarse, fine, basis_a, basis_b, keep, send1, recv1, send2, recv2,
           field_sem, load_sem, small_sem, halo_send, halo_recv,
           pick_send, pick_recv, s1_send, s1_recv, s2_send, s2_recv):
    rows, width = fbuf.shape
    half = width // 2
    bs = raw_main.shape[2]
    kc = 6
    nb = rows // bs
    groups = nb // GROUP
    ops = (ops0, ops1, ops2, ops3)
    re_bufs, im_bufs, ni_bufs = (re0, re1), (im0, im1), (ni0, ni1)
    me_d = lax.axis_index("depth")
    me_f = lax.axis_index("freq")
    first_row = me_d * rows
    core = lax.rem(me_f, 2)
    z = lax.rem(me_f // 2, NZH)
    y = lax.rem(me_f // (2 * NZH), NY)
    x = me_f // (2 * NZH * NY)
    sibling = me_f + 1 - 2 * core

    def chip_of(ox, oy, oz):
        return (lax.rem(x + ox, NX) * NY + lax.rem(y + oy, NY)) * NZH + lax.rem(z + oz, NZH)

    def device_of(ox, oy, oz, oc=0):
        return {"freq": chip_of(ox, oy, oz) * 2 + lax.rem(core + oc, 2)}

    fch = fbuf.shape[0] // groups

    def field_copy(g):
        at = pl.ds(pl.multiple_of(g * fch, fch), fch)
        return pltpu.make_async_copy(field_hbm.at[at], fbuf.at[at], field_sem.at[g])

    def ops_copies(g):
        at = pl.ds(g * GROUP, GROUP)
        return [pltpu.make_async_copy(src.at[at], dst.at[at], load_sem.at[which, g])
                for which, (src, dst) in enumerate(((main_hbm, raw_main), (side_hbm, raw_side)))]

    small = [pltpu.make_async_copy(src, dst, small_sem.at[i]) for i, (src, dst) in enumerate(
        ((coupling_hbm, coupling), (floors_hbm, floors), (freqs_hbm, freqs),
         (receivers_hbm, receivers)))]
    field_copy(0).start()
    field_copy(groups - 1).start()
    small[0].start()
    small[1].start()
    for copy in ops_copies(0):
        copy.start(priority=1)
    field_copy(1).start()

    def start_group(g, carry):
        field_copy(g + 1).start()
        for copy in ops_copies(g):
            copy.start(priority=1)
        return carry
    lax.fori_loop(1, groups - 2, start_group, 0)
    for g in (groups - 2, groups - 1):
        for copy in ops_copies(g):
            copy.start(priority=1)
    small[2].start()
    small[3].start()

    barrier = pltpu.get_barrier_semaphore()
    greeted = 0
    peers = [{"depth": 1 - me_d, "freq": me_f}, {"depth": 1 - me_d, "freq": sibling}]
    peers += [device_of(o, 0, 0) for o in range(1, NX)]
    peers += [device_of(0, o, oz) for o in range(NY) for oz in range(NZH) if o or oz]
    peers += [device_of(o, 0, oz, 1) for o in range(NX) for oz in range(NZH)]
    for peer in peers:
        pl.semaphore_signal(barrier, inc=1, device_id=peer, device_id_type=MESH)
        greeted += 1

    for buf in (final_re, final_im):
        buf[rows:, :] = jnp.zeros((buf.shape[0] - rows, half), F32)

    from_col = lax.broadcasted_iota(jnp.int32, (width, width), 0)
    to_col = lax.broadcasted_iota(jnp.int32, (width, width), 1)
    wanted = jnp.where(to_col < half, 2 * to_col, 2 * (to_col - half) + 1)
    order_buf[...] = jnp.where(from_col == wanted, 1.0, 0.0).astype(BF16)

    def put_w(parity, b, re, im):
        at = pl.ds(pl.multiple_of((b + 1) * bs, bs), bs)
        re_bufs[parity][at, :] = re
        im_bufs[parity][at, :] = im
        ni_bufs[parity][at, :] = -im

    zero_edge = jnp.zeros((bs, half), BF16)
    for buf in (re0, re1, im0, im1, ni0, ni1):
        buf[:bs, :] = zero_edge
        buf[(nb + 1) * bs:, :] = zero_edge

    def enter(g):
        at = pl.ds(pl.multiple_of(g * fch, fch), fch)
        got = jnp.dot(fbuf[at, :], order_buf[...], preferred_element_type=F32).astype(BF16)
        for i in range(GROUP):
            one = got[i * bs:(i + 1) * bs, :]
            put_w(0, g * GROUP + i, one[:, :half], one[:, half:])

    field_copy(0).wait()
    field_copy(groups - 1).wait()
    small[0].wait()
    small[1].wait()
    enter(0)
    enter(groups - 1)
    c16 = jnp.broadcast_to(coupling[...], (16, width))
    high = c16.astype(BF16)
    rest = c16 - high.astype(F32)
    mid = rest.astype(BF16)
    low = (rest - mid.astype(F32)).astype(BF16)
    three = jnp.dot(jnp.concatenate([high, mid, low], axis=0), order_buf[...],
                    preferred_element_type=F32)
    weights[...] = (three[:8] + three[16:24]) + three[32:40]

    below = 1 - me_d
    edge = pl.ds(pl.multiple_of((below * (nb - 1) + 1) * bs, bs), bs)

    def halo_copies(step):
        return [pltpu.make_async_remote_copy(
            src_ref=bufs[step % 2].at[edge],
            dst_ref=halo.at[step, which],
            send_sem=halo_send.at[step, which],
            recv_sem=halo_recv.at[step, which],
            device_id={"depth": 1 - me_d},
            device_id_type=MESH,
        ) for which, bufs in enumerate((re_bufs, im_bufs))]

    def halo_start(step):
        for copy in halo_copies(step):
            copy.start()

    def halo_wait(step):
        for copy in halo_copies(step):
            copy.wait()

    def halo_put(step):
        put_w(step % 2, below * (nb + 1) - 1, halo[step, 0], halo[step, 1])

    row_iota = lax.broadcasted_iota(jnp.int32, (bs, half), 0)

    def piece_of(step, g, i, p):
        if step > 0:
            return ops[i][g, p]
        pair = [raw.at[g * GROUP + i][pl.ds(p, bs, stride=kc), :] for raw in (raw_main, raw_side)]
        piece = jnp.concatenate(pair, axis=0)
        ops[i][g, p] = piece
        return piece

    def multiply(step, g, i):
        b = g * GROUP + i
        parity = step % 2
        acc = None
        for k in range(3):
            at = pl.ds(pl.multiple_of((b + k) * bs, bs), bs)
            re, im, ni = re_bufs[parity][at, :], im_bufs[parity][at, :], ni_bufs[parity][at, :]
            near = jnp.concatenate([jnp.concatenate([re, im], axis=1),
                                    jnp.concatenate([ni, re], axis=1)], axis=0)
            block = jnp.concatenate(
                [piece_of(step, g, i, 2 * k), piece_of(step, g, i, 2 * k + 1)], axis=1)
            part = jnp.dot(block, near, preferred_element_type=F32)
            acc = part if acc is None else acc + part
        m, c = acc[:bs], acc[bs:]
        wr = weights[0:1, :half]
        wi = weights[0:1, half:]
        re = m[:, :half] + wr * c[:, :half] - wi * c[:, half:]
        im = m[:, half:] + wr * c[:, half:] + wi * c[:, :half]
        damp = jnp.where(row_iota >= floors[step] - (first_row + b * bs), F32(0.5), F32(1.0))
        re = damp * re
        im = damp * im
        if step == STEPS - 1:
            at = pl.ds(pl.multiple_of(b * bs, bs), bs)
            final_re[at, :] = re
            final_im[at, :] = im
        else:
            put_w(1 - parity, b, re.astype(BF16), im.astype(BF16))

    def first_step(g, skip=0, last_field=None):
        for copy in ops_copies(g):
            copy.wait()
        if last_field is None:
            field_copy(g + 2).wait()
        for i in range(GROUP):
            if i >= skip:
                multiply(0, g, i)
        if last_field is None:
            enter(g + 2)

    field_copy(1).wait()
    enter(1)
    first_step(0, skip=1)
    first_step(1)
    pl.semaphore_wait(barrier, greeted)
    halo_start(0)

    def first_loop(g, carry):
        first_step(g)
        return carry

    lax.fori_loop(2, groups - 3, first_loop, 0)
    first_step(groups - 3, last_field=False)
    first_step(groups - 2, last_field=False)
    for copy in ops_copies(groups - 1):
        copy.wait()
    halo_wait(0)
    for i in range(GROUP - 1):
        multiply(0, groups - 1, i)
    halo_put(0)
    multiply(0, 0, 0)
    multiply(0, groups - 1, GROUP - 1)
    small[2].wait()
    small[3].wait()
    spot = receivers[...] - first_row
    inside = jnp.logical_and(spot >= 0, spot < rows)
    near_rows[...] = jnp.where(inside, spot, rows)
    spot_copies = [
        pltpu.make_async_copy(near_rows.at[j], spots.at[pl.ds(j * bs, bs)], small_sem.at[4 + j])
        for j in range(near_rows.shape[0])]
    for copy in spot_copies:
        copy.start()

    for step in range(1, STEPS):
        halo_start(step)
        for b in range(1, nb - 1 - LATE):
            multiply(step, b // GROUP, b % GROUP)
        halo_wait(step)
        for b in range(nb - 1 - LATE, nb - 1):
            multiply(step, b // GROUP, b % GROUP)
        halo_put(step)
        multiply(step, 0, 0)
        multiply(step, groups - 1, GROUP - 1)

    here = 2 * bs

    def pick(owner, side):
        base = owner * here + lax.rem(core + side, 2) * bs

        def take(q, carry):
            for j in range(16):
                row = q * 16 + j
                spot = spots[base + row]
                grab_re[pl.ds(row, 1), :] = final_re[pl.ds(spot, 1), :]
                grab_im[pl.ds(row, 1), :] = final_im[pl.ds(spot, 1), :]
            return carry

        lax.fori_loop(0, bs // 16, take, 0, unroll=2)
        return jnp.concatenate([grab_re[...], grab_im[...]], axis=1).astype(BF16)

    for copy in spot_copies:
        copy.wait()

    def move(src, dst, sems, at, to):
        return pltpu.make_async_remote_copy(
            src_ref=src, dst_ref=dst, send_sem=sems[0].at[at], recv_sem=sems[1].at[at],
            device_id=to, device_id_type=MESH)

    pick_sems = (pick_send, pick_recv)
    across = []
    for side, line in enumerate((me_f, sibling)):
        across.append(move(picked.at[side], pick_in.at[side], pick_sems, side,
                           {"depth": 1 - me_d, "freq": line}))
    beside = move(own.at[1], sib_own, pick_sems, 2, {"freq": sibling})
    for side in range(2):
        picked[side] = pick(1 - me_d, side)
        across[side].start()
    own[1] = pick(me_d, 1)
    beside.start()
    own[0] = pick(me_d, 0)

    chips = NX * NY * NZH
    times = NT // (2 * chips)
    count = lax.broadcasted_iota(jnp.int32, (chips, half), 0).astype(F32)
    late = lax.broadcasted_iota(jnp.int32, (2 * times, half), 0)
    late = jnp.where(late < times, late + core * times, late - core * times).astype(F32)
    for h, line in enumerate((me_f, sibling)):
        tone = freqs[pl.ds(line, 1), :]
        at = slice(h * half, (h + 1) * half)
        cos, sin = turn((tone * count) * F32(1.0 / chips))
        coarse[0, :, at] = cos
        coarse[1, :, at] = -sin
        cos, sin = turn((tone * late) * F32(1.0 / NT))
        fine[0, :, at] = cos
        fine[1, :, at] = sin
    th = times

    def place_of(off):
        return lax.rem(off, 2) * 2 + off // 2

    def basis_of(q, carry):
        ox, oy = q // NY, lax.rem(q, NY)
        for oz in range(NZH):
            chip = chip_of(ox, oy, oz)
            ca = coarse[0, pl.ds(chip, 1), :]
            na = coarse[1, pl.ds(chip, 1), :]
            for part, (basis, place) in enumerate(
                    ((basis_a, place_of(oy) * NX + ox), (basis_b, place_of(ox) * NY + oy))):
                at = pl.ds(pl.multiple_of((place * NZH + oz) * th, th), th)
                cb = fine[0, part * th:(part + 1) * th, :]
                sb = fine[1, part * th:(part + 1) * th, :]
                cos = (ca * cb + na * sb).astype(BF16)
                nsin = (na * cb - ca * sb).astype(BF16)
                for h in range(2):
                    basis[at, 2 * h * half:(2 * h + 1) * half] = cos[:, h * half:(h + 1) * half]
                    basis[at, (2 * h + 1) * half:(2 * h + 2) * half] = nsin[:, h * half:(h + 1) * half]
        return carry

    lax.fori_loop(0, NX * NY, basis_of, 0, unroll=2)

    for copy in across:
        copy.wait()
    beside.wait()
    for h, one in enumerate((own.at[0], sib_own)):
        owned[:, h * width:(h + 1) * width] = (
            one[...].astype(F32) + pick_in[h].astype(F32)).astype(BF16)

    slab = NY * NZH * th
    piece = NZH * th
    s1, s2 = (s1_send, s1_recv), (s2_send, s2_recv)

    def over(part, off):
        return device_of(off, 0, 0) if part == 0 else device_of(0, off, 0)

    def series(basis, at):
        return lax.dot_general(basis[at, :], owned[...], (((1,), (1,)), ((), ())),
                               preferred_element_type=F32)

    def first_copy(part, off, place):
        return move(send1.at[part, off - 1, place], recv1.at[part, off - 1, place], s1,
                    (part, off - 1, place), over(part, off))

    def second_copy(part, place, oz):
        off = (place % 2) * 2 + place // 2
        to = device_of(off, 0, oz, 1) if part else device_of(0, off, oz)
        return move(send2.at[part, place, oz], recv2.at[part, place, oz], s2,
                    (part, place, oz), to)

    for places in ((1,), (2, 3), (0,)):
        size = NX * piece
        for part, basis in enumerate((basis_a, basis_b)):
            got = series(basis, slice(places[0] * size, (places[-1] + 1) * size))
            for k, place in enumerate(places):
                keep[part, place] = got[k * size:k * size + piece]
                for off in range(1, NX):
                    send1[part, off - 1, place] = got[
                        k * size + off * piece:k * size + (off + 1) * piece].astype(BF16)
        for place in places:
            for off in (2, 1, 3):
                for part in range(2):
                    first_copy(part, off, place).start()

    for place in (1, 2, 3, 0):
        for part in range(2):
            for off in range(1, NX):
                first_copy(part, off, place).wait()
            total = keep[part, place]
            for k in range(NX - 1):
                total = total + recv1[part, k, place].astype(F32)
            for oz in (1, 0):
                one = total[oz * th:(oz + 1) * th]
                if part or place or oz:
                    send2[part, place, oz] = one.astype(BF16)
                    second_copy(part, place, oz).start()
                else:
                    keep[0, 0, :th, :] = one
    came = [(part, place, oz) for part in range(2) for place in range(NY) for oz in range(NZH)
            if part or place or oz]
    for at in came:
        second_copy(*at).wait()
    both = [keep[0, 0, :th, :], None]
    for part, place, oz in came:
        one = recv2[part, place, oz].astype(F32)
        both[part] = one if both[part] is None else both[part] + one
    mine, theirs = both[0] * factor, both[1] * factor
    first = core == 0
    out[:, :bs] = jnp.where(first, mine, theirs)
    out[:, bs:] = jnp.where(first, theirs, mine)


def local(depth_n, freq_n, pressure_field, block_main, block_coupled, coupling, frequencies,
          receivers, floors):
    rows, width = pressure_field.shape
    bs = block_main.shape[3]
    half = width // 2
    nb = rows // bs
    here = receivers.shape[0] // depth_n
    times = NT // freq_n
    factor = 1.0 / math.sqrt(frequencies.shape[0])
    vmem = pl.BlockSpec(memory_space=pltpu.VMEM)
    hbm = pl.BlockSpec(memory_space=pl.ANY)
    chips = NX * NY * NZH
    th = times
    slab = NY * NZH * th
    dma = pltpu.SemaphoreType.DMA
    result = pl.pallas_call(
        functools.partial(kernel, depth_n, factor),
        out_shape=jax.ShapeDtypeStruct((times, here), F32),
        in_specs=[hbm] * 7,
        out_specs=vmem,
        scratch_shapes=[
            pltpu.VMEM((rows, width), BF16),
            pltpu.VMEM((nb, 6 * bs, bs), BF16),
            pltpu.VMEM((nb, 6 * bs, bs), BF16),
            *[pltpu.VMEM((nb // GROUP, 6, 2 * bs, bs), BF16) for _ in range(GROUP)],
            *[pltpu.VMEM(((nb + 2) * bs, half), BF16) for _ in range(6)],
            pltpu.VMEM((rows + 8, half), F32),
            pltpu.VMEM((rows + 8, half), F32),
            pltpu.VMEM((STEPS, 2, bs, half), BF16),
            pltpu.VMEM((width, width), BF16),
            pltpu.VMEM((1, width), F32),
            pltpu.VMEM((frequencies.shape[0] // half, half), F32),
            pltpu.VMEM((receivers.shape[0] // bs, bs), jnp.int32),
            pltpu.SMEM((STEPS,), jnp.int32),
            pltpu.VMEM((8, width), F32),
            pltpu.VMEM((receivers.shape[0] // bs, bs), jnp.int32),
            pltpu.SMEM((receivers.shape[0],), jnp.int32),
            pltpu.VMEM((bs, half), F32),
            pltpu.VMEM((bs, half), F32),
            pltpu.VMEM((2, bs, width), BF16),
            pltpu.VMEM((2, bs, width), BF16),
            pltpu.VMEM((2, bs, width), BF16),
            pltpu.VMEM((bs, width), BF16),
            pltpu.VMEM((bs, 2 * width), BF16),
            pltpu.VMEM((2, chips, width), F32),
            pltpu.VMEM((2, 2 * times, width), F32),
            pltpu.VMEM((NX * slab, 2 * width), BF16),
            pltpu.VMEM((NX * slab, 2 * width), BF16),
            pltpu.VMEM((2, NY, NZH * th, bs), F32),
            pltpu.VMEM((2, NX - 1, NY, NZH * th, bs), BF16),
            pltpu.VMEM((2, NX - 1, NY, NZH * th, bs), BF16),
            pltpu.VMEM((2, NY, NZH, th, bs), BF16),
            pltpu.VMEM((2, NY, NZH, th, bs), BF16),
            dma((nb // GROUP,)),
            dma((2, nb // GROUP)),
            dma((4 + receivers.shape[0] // bs,)),
            dma((STEPS, 2)),
            dma((STEPS, 2)),
            dma((3,)),
            dma((3,)),
            dma((2, NX - 1, NY)),
            dma((2, NX - 1, NY)),
            dma((2, NY, NZH)),
            dma((2, NY, NZH)),
        ],
        compiler_params=pltpu.CompilerParams(
            collective_id=0, has_side_effects=True, vmem_limit_bytes=64 * 1024 * 1024 - 128 * 1024
        ),
    )(
        pressure_field,
        block_main.reshape(nb, 6 * bs, bs),
        block_coupled.reshape(nb, 6 * bs, bs),
        coupling.reshape(1, width),
        frequencies.reshape(-1, half),
        receivers.reshape(-1, bs),
        floors,
    )
    return result.T


def solution(mesh):
    in_specs = (
        P("depth", "freq"),
        P("depth", None, None, None),
        P("depth", None, None, None),
        P("freq"),
        P(),
        P(),
        P(),
    )
    body = functools.partial(local, mesh.shape["depth"], mesh.shape["freq"])
    return jax.shard_map(body, mesh=mesh, in_specs=in_specs, out_specs=P("depth", "freq"),
                         check_vma=False)
```
